32 devices in a mesh: dp: 1 (over z), sp: 32 (over x, y, core).
Axes of the slice: x: 4, y: 4, z: 1, core: 2. Of those that a mesh axis runs over, the one named last changes fastest.
The devices are a block of a 4x4x8 slice.
Arguments:
- x: bfloat16 [8192, 2048], P(('dp', 'sp'))
- gain: bfloat16 [2048], replicated
- wq: bfloat16 [2048, 2048], replicated
- wk: bfloat16 [2048, 256], replicated
- wv: bfloat16 [2048, 256], replicated
- wo: bfloat16 [2048, 2048], replicated
Outputs:
- output: bfloat16 [8192, 2048], P(('dp', 'sp'))
All inputs are finite; a program needn't handle non-finite values.
Results may differ from the reference program's by a relative error of at most 0.012.
Values are sent between devices in bfloat16 or wider.
A program may use at most 768 MiB of HBM per device.

```python
import jax
import jax.numpy as jnp
from jax import lax

ROWS = 8192
D = 2048
HEADS = 8
KV_HEADS = 1
HEAD = 256
THETA = 10000


def setup_inputs(seed: int = 0, part: int = 0) -> dict:
    kx, kn, kq, kk, kv, ko = jax.random.split(jax.random.key(seed), 6)

    def weights(key, rows, columns):
        return jax.random.normal(key, (rows, columns), jnp.float32) * rows**-0.5

    drawn = {
        "x": jax.random.normal(jax.random.fold_in(kx, part), (ROWS, D), jnp.float32),
        "gain": 1 + 0.1 * jax.random.normal(kn, (D,), jnp.float32),
        "wq": 2 * weights(kq, D, HEADS * HEAD),
        "wk": 2 * weights(kk, D, KV_HEADS * HEAD),
        "wv": 4 * weights(kv, D, KV_HEADS * HEAD),
        "wo": weights(ko, HEADS * HEAD, D),
    }
    return {k: v.astype(jnp.bfloat16) for k, v in drawn.items()}


def normed(x, gain):
    wide = x.astype(jnp.float32)
    scale = lax.rsqrt(jnp.mean(wide * wide, -1, keepdims=True) + 1e-6)
    return (wide * scale * gain.astype(jnp.float32)).astype(jnp.bfloat16)


def turned(t, place, theta):
    half = t.shape[-1] // 2
    angle = place.astype(jnp.float32)[:, None] * theta ** (-jnp.arange(half, dtype=jnp.float32) / half)
    cos, sin = jnp.cos(angle)[:, None], jnp.sin(angle)[:, None]
    a, b = t[..., :half].astype(jnp.float32), t[..., half:].astype(jnp.float32)
    return jnp.concatenate([a * cos - b * sin, b * cos + a * sin], -1).astype(jnp.bfloat16)


def matmul(a, w):
    return jnp.dot(a, w, preferred_element_type=jnp.float32).astype(jnp.bfloat16)


def einsum(form, a, b):
    return jnp.einsum(form, a.astype(jnp.float32), b.astype(jnp.float32))


def attention(q, k, v):
    scores = einsum("tgsd,ugd->gstu", q, k) * q.shape[-1] ** -0.5
    token = jnp.arange(q.shape[0])
    scores = jnp.where(token[:, None] >= token, scores, -jnp.inf)
    weights = jax.nn.softmax(scores, -1).astype(jnp.bfloat16)
    return einsum("gstu,ugd->tgsd", weights, v).astype(jnp.bfloat16)


def reference(x, gain, wq, wk, wv, wo):
    a, place = normed(x, gain), jnp.arange(ROWS)
    q = turned(matmul(a, wq).reshape(ROWS, HEADS, HEAD), place, THETA).reshape(ROWS, KV_HEADS, -1, HEAD)
    k = turned(matmul(a, wk).reshape(ROWS, KV_HEADS, HEAD), place, THETA)
    v = matmul(a, wv).reshape(ROWS, KV_HEADS, HEAD)
    seen = attention(q, k, v).reshape(ROWS, HEADS * HEAD)
    return (x.astype(jnp.float32) + jnp.dot(seen, wo, preferred_element_type=jnp.float32)).astype(jnp.bfloat16)
```

```python
import functools
import math

import jax
import jax.numpy as jnp
import numpy as np
from jax import lax
from jax.experimental import pallas as pl
from jax.experimental.pallas import tpu as pltpu
from jax.sharding import PartitionSpec as P

HEAD = 256
THETA = 10000
NEG = -1e30
HIDDEN = 2 * NEG
TOP = 3e38
LOG2E = 1.4426950408889634
MESH = pl.DeviceIdType.MESH
VMEM = 62 * 2**20
STRIP = 512

ORDER = ((0, 0), (-1, 0), (1, 0), (0, -1), (0, 1), (2, 0), (-1, -1), (-1, 1), (1, -1), (1, 1), (2, -1), (2, 1), (0, 2), (-1, 2), (1, 2), (2, 2))


def _dot(a, b, ca=1, cb=0):
    return lax.dot_general(a, b, (((ca,), (cb,)), ((), ())), preferred_element_type=jnp.float32)


def _rope(t, cos, sin):
    half = t.shape[-1] // 2
    t = t.astype(jnp.bfloat16).astype(jnp.float32)
    a, b = t[:, :half], t[:, half:]
    return jnp.concatenate([a * cos - b * sin, b * cos + a * sin], -1)


def _kernel(side, heads, x_hbm, gain_ref, freq_ref, wq_hbm, wk_hbm, wv_hbm, wo_hbm, y_hbm,
            x_v, a_v, wq_v, wk_v, wv_v, wo_v, q_v, blk, acc, top_s, s_a, s_b, cos_v, sin_v,
            in_sem, out_sem, ssem, rsem):
    own = x_v.shape[0]
    cols = heads * own
    e = HEAD**-0.5 * LOG2E
    me = lax.axis_index("sp")
    core = lax.rem(me, 2)
    chip = me // 2
    cx, cy = chip // side, lax.rem(chip, side)
    p = cx + (cy - cx) * core
    s = cy + (cx - cy) * core
    wide = 2 * side
    wp, ws = wide - (wide - 2) * core, 2 + (wide - 2) * core
    partner = me + 1 - 2 * core

    def at(a, b):
        return lax.rem(p + side + a, side) * wp + lax.rem(s + side + b, side) * ws + core

    def beside(a, b):
        return lax.rem(s + side + a, side) * ws + lax.rem(p + side + b, side) * wp + 1 - core

    def pick(k, f):
        if isinstance(k, int):
            return f(*ORDER[k])
        out = f(*ORDER[1])
        for n in range(2, len(ORDER)):
            out = jnp.where(k == n, f(*ORDER[n]), out)
        return out

    right_p, left_p, right_s, left_s = at(1, 0), at(-1, 0), at(0, 1), at(0, -1)

    loads = [pltpu.make_async_copy(src, dst, in_sem.at[n]) for n, (src, dst) in enumerate(
        ((x_hbm, x_v), (wk_hbm, wk_v), (wv_hbm, wv_v), (wq_hbm, wq_v), (wo_hbm, wo_v)))]
    for copy in loads:
        copy.start()
    barrier = pltpu.get_barrier_semaphore()
    for other in (right_p, left_p, right_s, left_s, partner):
        pl.semaphore_signal(barrier, inc=1, device_id={"sp": other}, device_id_type=MESH)

    place = (me * own + lax.broadcasted_iota(jnp.int32, (own, HEAD // 2), 0)).astype(jnp.float32)
    angle = place * freq_ref[...]
    cos_v[...] = jnp.cos(angle)
    sin_v[...] = jnp.sin(angle)

    loads[0].wait()
    x = x_v[...].astype(jnp.float32)
    scale = lax.rsqrt(jnp.mean(x * x, -1, keepdims=True) + 1e-6)
    a_v[...] = (x * scale * gain_ref[...].astype(jnp.float32)).astype(jnp.bfloat16)
    loads[1].wait()
    blk[me, 0] = _rope(_dot(a_v[...], wk_v[...]), cos_v[...], sin_v[...]).astype(jnp.bfloat16)
    loads[2].wait()
    blk[me, 1] = _dot(a_v[...], wv_v[...]).T.astype(jnp.bfloat16)

    sends = []

    def copy_of(block, part, other, send=0):
        ref = blk.at[block] if part is None else blk.at[block, part]
        return pltpu.make_async_remote_copy(src_ref=ref, dst_ref=ref, send_sem=ssem.at[send], recv_sem=rsem.at[block, part or 0],
                                            device_id={"sp": other}, device_id_type=MESH)

    def send(block, part, other):
        copy = copy_of(block, part, other, len(sends))
        sends.append(part)
        copy.start()

    def arrived(block, halves=False):
        if halves:
            copy_of(block, 0, partner).wait_recv()
            copy_of(block, 1, partner).wait_recv()
        else:
            copy_of(block, None, partner).wait_recv()

    pl.semaphore_wait(barrier, 5)
    send(me, None, right_p)
    send(me, None, left_p)
    send(me, None, partner)

    loads[3].wait()

    def project(h, _):
        here = pl.ds(pl.multiple_of(h * HEAD, HEAD), HEAD)
        q_v[:, here] = _rope(_dot(a_v[...], wq_v[:, here]), cos_v[...], sin_v[...]).T.astype(jnp.bfloat16)
        return _

    lax.fori_loop(0, heads, project, None)

    for n in (0, 1):
        copy_of(me, None, partner, n).wait_send()
    send(me, None, right_s)
    send(me, None, left_s)

    def exchange(k):
        a, b = ORDER[k]
        block = at(a, b)
        arrived(block, halves=b == 2 or (a, b) == (2, 0))
        if b == 0:
            if a != 2:
                send(block, 0 if a < 0 else 1, right_p if a < 0 else left_p)
            send(block, None, right_s)
            send(block, None, left_s)
        elif b != 2:
            send(block, 0 if b < 0 else 1, right_s if b < 0 else left_s)
        send(block, None, partner)

    strips = range(0, cols, STRIP)

    def scores(k, out):
        first, second = pick(k, at), pick(k, beside)
        for c in strips:
            q = q_v[:, c : c + STRIP]
            out[:own, c : c + STRIP] = _dot(blk[first, 0], q)
            out[own:, c : c + STRIP] = _dot(blk[second, 0], q)

    def attend(k, sc, first_step=False):
        first, second = pick(k, at), pick(k, beside)
        seen0, seen1 = (first < me), (second < me)
        most0, most1 = jnp.where(seen0, TOP, NEG), jnp.where(seen1, TOP, NEG)
        cap0, cap1 = jnp.where(seen0, 1.0, 0.0), jnp.where(seen1, 1.0, 0.0)
        values = jnp.concatenate([blk[first, 1], blk[second, 1]], axis=1)
        values = jnp.concatenate([values, jnp.ones((8, 2 * own), jnp.bfloat16)], axis=0)
        for c in strips:
            s0, s1 = sc[:own, c : c + STRIP], sc[own:, c : c + STRIP]
            if first_step:
                ok = lax.rem(lax.broadcasted_iota(jnp.int32, (own, STRIP), 1), own) >= lax.broadcasted_iota(jnp.int32, (own, STRIP), 0)
                s0 = jnp.where(ok, s0, HIDDEN)
                m = s0.max(axis=0, keepdims=True)
            else:
                m = jnp.minimum(s0.max(axis=0, keepdims=True), most0)
            m = jnp.maximum(m, jnp.minimum(s1.max(axis=0, keepdims=True), most1))
            if first_step:
                top = m
            else:
                old = top_s[:, c : c + STRIP]
                top = jnp.maximum(old, m)
                keep = jnp.exp2((old - top) * e)
            top_s[:, c : c + STRIP] = top
            p0 = jnp.exp2((s0 - top) * e).astype(jnp.bfloat16)
            p1 = jnp.exp2((s1 - top) * e).astype(jnp.bfloat16)
            if not first_step:
                p0 = jnp.minimum(p0, cap0.astype(jnp.bfloat16))
            p1 = jnp.minimum(p1, cap1.astype(jnp.bfloat16))
            got = _dot(values, jnp.concatenate([p0, p1], axis=0))
            acc[:, c : c + STRIP] = got if first_step else acc[:, c : c + STRIP] * keep + got

    last = len(ORDER) - 1
    arrived(partner)
    scores(0, s_a)
    exchange(1)
    arrived(beside(*ORDER[1]))
    scores(1, s_b)
    attend(0, s_a, first_step=True)

    def pair(t, _):
        for odd in (0, 1):
            k = 1 + odd + 2 * t
            for n in range(2 + odd, last + 1, 2):
                pl.when(k + 1 == n)(functools.partial(exchange, n))
            arrived(pick(k + 1, beside))
            now, later = (s_a, s_b) if odd else (s_b, s_a)
            scores(k + 1, later)
            attend(k, now)
        return _

    lax.fori_loop(0, (last - 1) // 2, pair, None)
    attend(last, s_b)

    for h in range(heads):
        here = slice(h * own, (h + 1) * own)
        out = acc[:HEAD, here] * (1 / acc[HEAD : HEAD + 1, here])
        a_v[:, h * HEAD : (h + 1) * HEAD] = out.T.astype(jnp.bfloat16)

    loads[4].wait()
    chunk = 512

    def result(n, _):
        here = pl.ds(pl.multiple_of(n * chunk, chunk), chunk)
        y = _dot(a_v[...], wo_v[:, here])
        x_v[:, here] = (x_v[:, here].astype(jnp.float32) + y).astype(jnp.bfloat16)
        pltpu.make_async_copy(x_v.at[:, here], y_hbm.at[:, here], out_sem.at[n]).start()
        return _

    assert len(sends) == 36, len(sends)
    chunks = x_v.shape[1] // chunk
    lax.fori_loop(0, chunks, result, None)
    for n, part in enumerate(sends):
        if n >= 2:
            copy_of(me, part, partner, n).wait_send()
    for n in range(chunks):
        here = pl.ds(n * chunk, chunk)
        pltpu.make_async_copy(x_v.at[:, here], y_hbm.at[:, here], out_sem.at[n]).wait()


def solution(mesh):
    side = math.isqrt(mesh.shape["sp"] // 2)

    def step(x, gain, wq, wk, wv, wo):
        own, d = x.shape
        heads = wq.shape[1] // HEAD
        cols = heads * own
        n = mesh.shape["sp"]
        freq = jnp.asarray(np.float32(THETA) ** (-np.arange(HEAD // 2, dtype=np.float32) / np.float32(HEAD // 2)))[None]
        hbm, vmem = pl.BlockSpec(memory_space=pl.ANY), pl.BlockSpec(memory_space=pltpu.VMEM)
        bf16, f32 = jnp.bfloat16, jnp.float32
        return pl.pallas_call(
            functools.partial(_kernel, side, heads),
            in_specs=[hbm, vmem, vmem, hbm, hbm, hbm, hbm],
            out_specs=hbm,
            out_shape=jax.ShapeDtypeStruct((own, d), bf16),
            scratch_shapes=[
                pltpu.VMEM((own, d), bf16),
                pltpu.VMEM((own, d), bf16),
                pltpu.VMEM(wq.shape, bf16),
                pltpu.VMEM(wk.shape, bf16),
                pltpu.VMEM(wv.shape, bf16),
                pltpu.VMEM(wo.shape, bf16),
                pltpu.VMEM((HEAD, cols), bf16),
                pltpu.VMEM((n, 2, own, HEAD), bf16),
                pltpu.VMEM((HEAD + 8, cols), f32),
                pltpu.VMEM((1, cols), f32),
                pltpu.VMEM((2 * own, cols), f32),
                pltpu.VMEM((2 * own, cols), f32),
                pltpu.VMEM((own, HEAD // 2), f32),
                pltpu.VMEM((own, HEAD // 2), f32),
                pltpu.SemaphoreType.DMA((5,)),
                pltpu.SemaphoreType.DMA((8,)),
                pltpu.SemaphoreType.DMA((64,)),
                pltpu.SemaphoreType.DMA((n, 2)),
            ],
            compiler_params=pltpu.CompilerParams(collective_id=0, has_side_effects=True, vmem_limit_bytes=VMEM),
        )(x, gain[None], freq, wq, wk, wv, wo)

    tokens, whole = P(("dp", "sp"), None), P(None, None)
    return jax.shard_map(step, mesh=mesh, in_specs=(tokens, P(None), whole, whole, whole, whole), out_specs=tokens, check_vma=False)
```

```python
import functools
import math

import jax
import jax.numpy as jnp
import numpy as np
from jax import lax
from jax.experimental import pallas as pl
from jax.experimental.pallas import tpu as pltpu
from jax.sharding import PartitionSpec as P

HEAD = 256
THETA = 10000
NEG = -1e30
HIDDEN = 2 * NEG
LOG2E = 1.4426950408889634
MESH = pl.DeviceIdType.MESH
VMEM = 62 * 2**20
STRIP = 512
WIDE = 512

ORDER = ((0, 0), (-1, 0), (1, 0), (0, -1), (0, 1), (2, 0), (-1, -1), (-1, 1), (1, -1), (1, 1), (2, -1), (2, 1), (0, 2), (-1, 2), (1, 2), (2, 2))


def _dot(a, b, ca=1, cb=0):
    return lax.dot_general(a, b, (((ca,), (cb,)), ((), ())), preferred_element_type=jnp.float32)


def _rope(t, cos, sin):
    half = t.shape[-1] // 2
    t = t.astype(jnp.bfloat16).astype(jnp.float32)
    a, b = t[:, :half], t[:, half:]
    return jnp.concatenate([a * cos - b * sin, b * cos + a * sin], -1)


def _kernel(side, heads, x_hbm, gain_ref, freq_ref, wq_hbm, wk_hbm, wv_hbm, wo_hbm, y_hbm,
            x_v, a_v, wq_v, wkv_v, wo_v, q_v, blk, acc, top_s, s_a, s_b, m_a, m_b, cos_v, sin_v,
            in_sem, out_sem, ssem, rsem):
    own, d = x_v.shape
    cols = heads * own
    e = HEAD**-0.5 * LOG2E
    me = lax.axis_index("sp")
    core = lax.rem(me, 2)
    chip = lax.div(me, 2)
    cx, cy = lax.div(chip, side), lax.rem(chip, side)
    p = cx + (cy - cx) * core
    s = cy + (cx - cy) * core
    wide = 2 * side
    wp, ws = wide - (wide - 2) * core, 2 + (wide - 2) * core
    partner = me + 1 - 2 * core

    def at(a, b):
        return lax.rem(p + side + a, side) * wp + lax.rem(s + side + b, side) * ws + core

    def beside(a, b):
        return lax.rem(s + side + a, side) * ws + lax.rem(p + side + b, side) * wp + 1 - core

    def pick(k, f):
        if isinstance(k, int):
            return f(*ORDER[k])
        out = f(*ORDER[1])
        for n in range(2, len(ORDER)):
            out = jnp.where(k == n, f(*ORDER[n]), out)
        return out

    right_p, left_p, right_s, left_s = at(1, 0), at(-1, 0), at(0, 1), at(0, -1)

    load_x = pltpu.make_async_copy(x_hbm, x_v, in_sem.at[0])
    load_k = pltpu.make_async_copy(wk_hbm, wkv_v.at[:, pl.ds(0, HEAD)], in_sem.at[1])
    load_v = pltpu.make_async_copy(wv_hbm, wkv_v.at[:, pl.ds(HEAD, HEAD)], in_sem.at[2])
    load_o = pltpu.make_async_copy(wo_hbm, wo_v, in_sem.at[3])

    def load_q(n):
        here = pl.ds(n * WIDE if isinstance(n, int) else pl.multiple_of(n * WIDE, WIDE), WIDE)
        return pltpu.make_async_copy(wq_hbm.at[:, here], wq_v.at[:, here], in_sem.at[4 + n])

    load_x.start()
    load_k.start()
    load_v.start()
    barrier = pltpu.get_barrier_semaphore()
    for other in (right_p, left_p, right_s, left_s, partner):
        pl.semaphore_signal(barrier, inc=1, device_id={"sp": other}, device_id_type=MESH)

    place = (me * own + lax.broadcasted_iota(jnp.int32, (own, HEAD // 2), 0)).astype(jnp.float32)
    angle = place * freq_ref[...]
    cos_v[...] = jnp.cos(angle)
    sin_v[...] = jnp.sin(angle)

    load_x.wait()
    for n in range(cols // WIDE):
        load_q(n).start()
    x = x_v[...].astype(jnp.float32)
    scale = lax.rsqrt(jnp.mean(x * x, -1, keepdims=True) + 1e-6)
    a_v[...] = (x * scale * gain_ref[...].astype(jnp.float32)[None]).astype(jnp.bfloat16)
    load_k.wait()
    load_v.wait()
    kv = _dot(a_v[...], wkv_v[...])
    blk[me, 0] = _rope(kv[:, :HEAD], cos_v[...], sin_v[...]).astype(jnp.bfloat16)
    blk[me, 1] = kv[:, HEAD:].T.astype(jnp.bfloat16)

    def copy_of(block, part, other, send=1):
        ref = blk.at[block] if part is None else blk.at[block, part]
        arrival = rsem.at[0, 0] if isinstance(block, pl.Slice) else rsem.at[block, part or 0]
        return pltpu.make_async_remote_copy(src_ref=ref, dst_ref=ref, send_sem=ssem.at[send], recv_sem=arrival,
                                            device_id={"sp": other}, device_id_type=MESH)

    def send(block, part, other):
        copy_of(block, part, other).start()

    def arrived(block, halves=False):
        if halves:
            copy_of(block, 0, partner).wait_recv()
            copy_of(block, 1, partner).wait_recv()
        else:
            copy_of(block, None, partner).wait_recv()

    pl.semaphore_wait(barrier, 5)
    first_sends = [copy_of(me, None, right_p, 0), copy_of(me, None, left_p, 2)]
    for copy in first_sends:
        copy.start()
    send(me, None, partner)

    def project(n, _):
        load_q(n).wait()
        here = pl.ds(pl.multiple_of(n * WIDE, WIDE), WIDE)
        q = _dot(a_v[...], wq_v[:, here])
        for h in range(WIDE // HEAD):
            turned = _rope(q[:, h * HEAD : (h + 1) * HEAD], cos_v[...], sin_v[...])
            q_v[:, pl.ds(pl.multiple_of(n * WIDE + h * HEAD, HEAD), HEAD)] = turned.T.astype(jnp.bfloat16)
        return _

    lax.fori_loop(0, cols // WIDE, project, None)
    load_o.start()

    for copy in first_sends:
        copy.wait_send()
    send(me, None, right_s)
    send(me, None, left_s)

    def exchange(k):
        a, b = ORDER[k]
        block = at(a, b)
        arrived(block, halves=b == 2 or (a, b) == (2, 0))
        if b == 0:
            if a != 2:
                send(block, 0 if a < 0 else 1, right_p if a < 0 else left_p)
            send(block, None, right_s)
            send(block, None, left_s)
        elif b != 2:
            send(block, 0 if b < 0 else 1, right_s if b < 0 else left_s)
        send(block, None, partner)

    strips = range(0, cols, STRIP)

    def scores(k, out, most):
        for n, block in enumerate((pick(k, at), pick(k, beside))):
            for c in strips:
                sc = _dot(blk[block, 0], q_v[:, c : c + STRIP]) * e
                out[n * own : (n + 1) * own, c : c + STRIP] = sc
                most[n : n + 1, c : c + STRIP] = sc.max(axis=0, keepdims=True)

    def attend(k, sc, most, masked, first_step=False):
        blocks = pick(k, at), pick(k, beside)
        values = jnp.concatenate([blk[blocks[0], 1], blk[blocks[1], 1]], axis=1)
        values = jnp.concatenate([values, jnp.ones((8, 2 * own), jnp.bfloat16)], axis=0)
        for c in strips:
            here = slice(c, c + STRIP)
            parts = [sc[:own, here], sc[own:, here]]
            tops = [most[:1, here], most[1:2, here]]
            if first_step:
                ok = lax.rem(lax.broadcasted_iota(jnp.int32, (own, STRIP), 1), own) >= lax.broadcasted_iota(jnp.int32, (own, STRIP), 0)
                parts[0] = jnp.where(ok, parts[0], HIDDEN)
                tops[0] = parts[0].max(axis=0, keepdims=True)
            if masked:
                tops = [jnp.where(block <= me, t, NEG) for block, t in zip(blocks, tops)]
            top = jnp.maximum(*tops)
            if not first_step:
                old = top_s[:, here]
                top = jnp.maximum(old, top)
                keep = jnp.exp2(old - top)
            top_s[:, here] = top
            weights = [jnp.exp2(t - top).astype(jnp.bfloat16) for t in parts]
            if masked:
                weights = [jnp.minimum(w, jnp.where(block <= me, 1.0, 0.0).astype(jnp.bfloat16)) for block, w in zip(blocks, weights)]
            got = _dot(values, jnp.concatenate(weights, axis=0))
            acc[:, here] = got if first_step else acc[:, here] * keep + got

    last = len(ORDER) - 1

    def seen(k):
        one, two = pick(k, at) < me, pick(k, beside) < me
        return one & two, one | two

    arrived(partner)
    scores(0, s_a, m_a)
    exchange(1)
    exchange(2)
    arrived(beside(*ORDER[1]))
    scores(1, s_b, m_b)
    attend(0, s_a, m_a, True, first_step=True)

    def pair(t, _):
        for odd in (0, 1):
            k = 1 + odd + 2 * t
            for n in range(3 + odd, last + 1, 2):
                pl.when(k + 2 == n)(functools.partial(exchange, n))
            arrived(pick(k + 1, beside))
            now, later = ((s_a, m_a), (s_b, m_b)) if odd else ((s_b, m_b), (s_a, m_a))
            every, some = seen(k)
            _, ahead = seen(k + 1)

            @pl.when(every)
            def _():
                scores(k + 1, *later)
                attend(k, *now, False)

            @pl.when(some & ~every)
            def _():
                scores(k + 1, *later)
                attend(k, *now, True)

            @pl.when(ahead & ~some)
            def _():
                scores(k + 1, *later)

        return _

    lax.fori_loop(0, (last - 1) // 2, pair, None)
    every, some = seen(last)
    pl.when(every)(functools.partial(attend, last, s_b, m_b, False))
    pl.when(some & ~every)(functools.partial(attend, last, s_b, m_b, True))

    for h in range(heads):
        here = slice(h * own, (h + 1) * own)
        out = acc[:HEAD, here] * (1 / acc[HEAD : HEAD + 1, here])
        a_v[:, h * HEAD : (h + 1) * HEAD] = out.T.astype(jnp.bfloat16)

    load_o.wait()

    def result(n):
        here = pl.ds(n * WIDE, WIDE)
        return pltpu.make_async_copy(x_v.at[:, here], y_hbm.at[:, here], out_sem.at[n])

    for n in range(d // WIDE):
        here = slice(n * WIDE, (n + 1) * WIDE)
        x_v[:, here] = (x_v[:, here].astype(jnp.float32) + _dot(a_v[...], wo_v[:, here])).astype(jnp.bfloat16)
        result(n).start()
    sent = 2 * len(ORDER) - 3
    copy_of(pl.ds(0, sent), None, partner).wait_send()
    for n in range(d // WIDE):
        result(n).wait()


def solution(mesh):
    side = math.isqrt(mesh.shape["sp"] // 2)

    def step(x, gain, wq, wk, wv, wo):
        own, d = x.shape
        heads = wq.shape[1] // HEAD
        cols = heads * own
        n = mesh.shape["sp"]
        freq = jnp.asarray(np.float32(THETA) ** (-np.arange(HEAD // 2, dtype=np.float32) / np.float32(HEAD // 2)))[None]
        hbm, vmem = pl.BlockSpec(memory_space=pl.ANY), pl.BlockSpec(memory_space=pltpu.VMEM)
        bf16, f32 = jnp.bfloat16, jnp.float32
        return pl.pallas_call(
            functools.partial(_kernel, side, heads),
            in_specs=[hbm, vmem, vmem, hbm, hbm, hbm, hbm],
            out_specs=hbm,
            out_shape=jax.ShapeDtypeStruct((own, d), bf16),
            scratch_shapes=[
                pltpu.VMEM((own, d), bf16),
                pltpu.VMEM((own, d), bf16),
                pltpu.VMEM(wq.shape, bf16),
                pltpu.VMEM((d, 2 * HEAD), bf16),
                pltpu.VMEM(wo.shape, bf16),
                pltpu.VMEM((HEAD, cols), bf16),
                pltpu.VMEM((n, 2, own, HEAD), bf16),
                pltpu.VMEM((HEAD + 8, cols), f32),
                pltpu.VMEM((1, cols), f32),
                pltpu.VMEM((2 * own, cols), f32),
                pltpu.VMEM((2 * own, cols), f32),
                pltpu.VMEM((2, cols), f32),
                pltpu.VMEM((2, cols), f32),
                pltpu.VMEM((own, HEAD // 2), f32),
                pltpu.VMEM((own, HEAD // 2), f32),
                pltpu.SemaphoreType.DMA((12,)),
                pltpu.SemaphoreType.DMA((8,)),
                pltpu.SemaphoreType.DMA((3,)),
                pltpu.SemaphoreType.DMA((n, 2)),
            ],
            compiler_params=pltpu.CompilerParams(collective_id=0, has_side_effects=True, vmem_limit_bytes=VMEM),
        )(x, gain, freq, wq, wk, wv, wo)

    tokens, whole = P(("dp", "sp"), None), P(None, None)
    return jax.shard_map(step, mesh=mesh, in_specs=(tokens, P(None), whole, whole, whole, whole), out_specs=tokens, check_vma=False)
```

```python
import functools
import math

import jax
import jax.numpy as jnp
from jax import lax
from jax.experimental import pallas as pl
from jax.experimental.pallas import tpu as pltpu
from jax.sharding import PartitionSpec as P

HEAD = 256
THETA = 10000
NEG = -1e30
HIDDEN = 2 * NEG
LOG2E = 1.4426950408889634
MESH = pl.DeviceIdType.MESH
VMEM = 38 * 2**20
STRIP = 512
WIDE = 512

ORDER = ((0, 0), (-1, 0), (1, 0), (0, -1), (0, 1), (2, 0), (-1, -1), (-1, 1), (1, -1), (1, 1), (0, 2), (2, -1), (2, 1), (-1, 2), (1, 2), (2, 2))
CHIPS = ((0, 0), (-1, 0), (0, -1), (1, 0), (0, 1), (-1, -1), (-1, 1), (1, -1), (1, 1), (2, 0), (0, 2), (2, -1), (-1, 2), (2, 1), (1, 2), (2, 2))
TAKEN = {2: (6,), 3: (7, 5), 4: (8,), 5: (9,), 6: (10,), 8: (11,), 9: (12, 13), 11: (14,), 13: (15,)}


def _dot(a, b, ca=1, cb=0):
    return lax.dot_general(a, b, (((ca,), (cb,)), ((), ())), preferred_element_type=jnp.float32)


def _rope(t, cos, sin):
    half = t.shape[-1] // 2
    t = t.astype(jnp.bfloat16).astype(jnp.float32)
    a, b = t[:, :half], t[:, half:]
    return jnp.concatenate([a * cos - b * sin, b * cos + a * sin], -1)


def _kernel(side, heads, x_hbm, gain_hbm, wq_hbm, wk_hbm, wv_hbm, wo_hbm, out_ref, x_v, wo_v,
            a_v, wq_v, wkv_v, q_v, blk, acc, top_s, s_a, s_b, m_a, m_b, cos_v, sin_v, gain_v,
            in_sem, ssem, rsem):
    own, d = x_v.shape
    cols = heads * own
    e = HEAD**-0.5 * LOG2E
    me = lax.axis_index("sp")
    core = lax.rem(me, 2)
    chip = lax.div(me, 2)
    cx, cy = lax.div(chip, side), lax.rem(chip, side)
    p = cx + (cy - cx) * core
    s = cy + (cx - cy) * core
    wide = 2 * side
    wp, ws = wide - (wide - 2) * core, 2 + (wide - 2) * core
    partner = me + 1 - 2 * core

    def at(a, b):
        return lax.rem(p + side + a, side) * wp + lax.rem(s + side + b, side) * ws + core

    def chip_at(x, y):
        return lax.rem(cx + side + x, side) * side + lax.rem(cy + side + y, side)

    def chip_of(k):
        if isinstance(k, int):
            return chip_at(*CHIPS[k])
        out = chip_at(*CHIPS[1])
        for n in range(2, len(CHIPS)):
            out = jnp.where(k == n, chip_at(*CHIPS[n]), out)
        return out

    right_p, left_p, right_s, left_s = at(1, 0), at(-1, 0), at(0, 1), at(0, -1)

    load_x = pltpu.make_async_copy(x_hbm, x_v, in_sem.at[0])
    load_k = pltpu.make_async_copy(wk_hbm, wkv_v.at[:, pl.ds(0, HEAD)], in_sem.at[1])
    load_v = pltpu.make_async_copy(wv_hbm, wkv_v.at[:, pl.ds(HEAD, HEAD)], in_sem.at[2])

    load_o = pltpu.make_async_copy(wo_hbm, wo_v, in_sem.at[3])

    def load_q(n):
        here = pl.ds(n * WIDE if isinstance(n, int) else pl.multiple_of(n * WIDE, WIDE), WIDE)
        return pltpu.make_async_copy(wq_hbm.at[:, here], wq_v.at[:, here], in_sem.at[4 + n])

    load_g = pltpu.make_async_copy(gain_hbm, gain_v, in_sem.at[11])
    load_x.start()
    load_g.start()
    load_k.start()
    load_v.start()
    barrier = pltpu.get_barrier_semaphore()
    for other in (right_p, left_p, right_s, left_s, partner):
        pl.semaphore_signal(barrier, inc=1, device_id={"sp": other}, device_id_type=MESH)

    place = (me * own + lax.broadcasted_iota(jnp.int32, (own, HEAD // 2), 0)).astype(jnp.float32)
    half = HEAD // 2
    angle = place * jnp.exp2(lax.broadcasted_iota(jnp.int32, (1, half), 1).astype(jnp.float32) * (-math.log2(THETA) / half))
    cos_v[...] = jnp.cos(angle)
    sin_v[...] = jnp.sin(angle)

    load_x.wait()
    load_g.wait()
    for n in range(cols // WIDE):
        load_q(n).start()
    x = x_v[...].astype(jnp.float32)
    scale = lax.rsqrt(jnp.mean(x * x, -1, keepdims=True) + 1e-6)
    a_v[...] = (x * scale * gain_v[...].astype(jnp.float32)[None]).astype(jnp.bfloat16)
    load_k.wait()
    load_v.wait()
    kv = _dot(a_v[...], wkv_v[...])
    blk[me, 0] = _rope(kv[:, :HEAD], cos_v[...], sin_v[...]).astype(jnp.bfloat16)
    blk[me, 1] = kv[:, HEAD:].T.astype(jnp.bfloat16)

    def copy_of(block, part, other, send=1):
        ref = blk.at[block] if part is None else blk.at[block, part]
        arrival = rsem.at[0, 0] if isinstance(block, pl.Slice) else rsem.at[block, part or 0]
        return pltpu.make_async_remote_copy(src_ref=ref, dst_ref=ref, send_sem=ssem.at[send], recv_sem=arrival,
                                            device_id={"sp": other}, device_id_type=MESH)

    def send(block, part, other):
        copy_of(block, part, other).start()

    def arrived(block, halves=False):
        if halves:
            copy_of(block, 0, partner).wait_recv()
            copy_of(block, 1, partner).wait_recv()
        else:
            copy_of(block, None, partner).wait_recv()

    pl.semaphore_wait(barrier, 5)
    first_sends = [copy_of(me, None, right_p, 0), copy_of(me, None, left_p, 2)]
    for copy in first_sends:
        copy.start()
    send(me, None, partner)

    def project(n, _):
        load_q(n).wait()
        here = pl.ds(pl.multiple_of(n * WIDE, WIDE), WIDE)
        q = _dot(a_v[...], wq_v[:, here])
        for h in range(WIDE // HEAD):
            turned = _rope(q[:, h * HEAD : (h + 1) * HEAD], cos_v[...], sin_v[...])
            q_v[:, pl.ds(pl.multiple_of(n * WIDE + h * HEAD, HEAD), HEAD)] = turned.T.astype(jnp.bfloat16)
        return _

    lax.fori_loop(0, cols // WIDE - 1, project, None)
    load_o.start()
    for copy in first_sends:
        copy.wait_send()
    send(me, None, right_s)
    send(me, None, left_s)
    lax.fori_loop(cols // WIDE - 1, cols // WIDE, project, None)

    def exchange(k):
        a, b = ORDER[k]
        block = at(a, b)
        arrived(block, halves=b == 2 or (a, b) == (2, 0))
        if b == 0:
            send(block, None, right_s)
            send(block, None, left_s)
        elif b != 2:
            send(block, 0 if b < 0 else 1, right_s if b < 0 else left_s)
        send(block, None, partner)
        if k == 4:
            send(at(-1, 0), 0, right_p)
            send(at(1, 0), 1, left_p)

    strips = range(0, cols, STRIP)

    def scores(k, out, most):
        chip = chip_of(k)
        for n in (0, 1):
            for c in strips:
                sc = _dot(blk[2 * chip + n, 0], q_v[:, c : c + STRIP]) * e
                out[n * own : (n + 1) * own, c : c + STRIP] = sc
                most[n : n + 1, c : c + STRIP] = sc.max(axis=0, keepdims=True)

    def attend(k, sc, most):
        chip = chip_of(k)
        values = jnp.concatenate([blk[2 * chip, 1], blk[2 * chip + 1, 1]], axis=1)
        values = jnp.concatenate([values, jnp.ones((8, 2 * own), jnp.bfloat16)], axis=0)
        first_step = isinstance(k, int) and k == 0
        for c in strips:
            here = slice(c, c + STRIP)
            weights = sc[:, here]
            if first_step:
                query = core * own + lax.rem(lax.broadcasted_iota(jnp.int32, (2 * own, STRIP), 1), own)
                weights = jnp.where(query >= lax.broadcasted_iota(jnp.int32, (2 * own, STRIP), 0), weights, HIDDEN)
                top = weights.max(axis=0, keepdims=True)
            else:
                old = top_s[:, here]
                top = jnp.maximum(old, jnp.maximum(most[:1, here], most[1:2, here]))
                keep = jnp.exp2(old - top)
            top_s[:, here] = top
            got = _dot(values, jnp.exp2(weights - top).astype(jnp.bfloat16))
            acc[:, here] = got if first_step else acc[:, here] * keep + got

    last = len(CHIPS) - 1

    def other_block(k):
        return 2 * chip_of(k) + 1 - core

    arrived(partner)
    scores(0, s_a, m_a)
    exchange(1)
    exchange(2)
    attend(0, s_a, m_a)
    exchange(3)
    exchange(4)
    arrived(other_block(1))
    scores(1, s_b, m_b)

    def pair(t, _):
        for odd in (0, 1):
            k = 1 + odd + 2 * t
            for n, taken in TAKEN.items():
                if n % 2 != odd:
                    @pl.when(k == n)
                    def _():
                        for r in taken:
                            exchange(r)
            arrived(other_block(k + 1))
            now, later = ((s_a, m_a), (s_b, m_b)) if odd else ((s_b, m_b), (s_a, m_a))
            seen, ahead = chip_of(k) < chip, chip_of(k + 1) < chip

            @pl.when(seen)
            def _():
                scores(k + 1, *later)
                attend(k, *now)

            @pl.when(ahead & ~seen)
            def _():
                scores(k + 1, *later)

        return _

    lax.fori_loop(0, (last - 1) // 2, pair, None)
    pl.when(chip_of(last) < chip)(functools.partial(attend, last, s_b, m_b))

    for h in range(heads):
        here = slice(h * own, (h + 1) * own)
        out = acc[:HEAD, here] * (1 / acc[HEAD : HEAD + 1, here])
        out_ref[:, h * HEAD : (h + 1) * HEAD] = out.T.astype(jnp.bfloat16)

    load_o.wait()
    sent = 2 * len(ORDER) - 3
    copy_of(pl.ds(0, sent), None, partner).wait_send()


def _finish(a_ref, x_ref, wo_ref, y_hbm, y_v, out_sem):
    def result(n):
        here = pl.ds(n * WIDE, WIDE)
        return pltpu.make_async_copy(y_v.at[:, here], y_hbm.at[:, here], out_sem.at[n])

    chunks = range(x_ref.shape[1] // WIDE)
    for n in chunks:
        here = slice(n * WIDE, (n + 1) * WIDE)
        y_v[:, here] = (x_ref[:, here].astype(jnp.float32) + _dot(a_ref[...], wo_ref[:, here])).astype(jnp.bfloat16)
        result(n).start()
    for n in chunks:
        result(n).wait()


def solution(mesh):
    side = math.isqrt(mesh.shape["sp"] // 2)

    def step(x, gain, wq, wk, wv, wo):
        own, d = x.shape
        heads = wq.shape[1] // HEAD
        cols = heads * own
        n = mesh.shape["sp"]
        hbm, vmem = pl.BlockSpec(memory_space=pltpu.HBM), pl.BlockSpec(memory_space=pltpu.VMEM)
        bf16, f32 = jnp.bfloat16, jnp.float32
        x_h, wq_h, wk_h, wv_h, wo_h = (pltpu.with_memory_space_constraint(t, pltpu.HBM) for t in (x, wq, wk, wv, wo))
        gain_h = pltpu.with_memory_space_constraint(gain, pltpu.HBM)
        attended, x_in, wo_in = pl.pallas_call(
            functools.partial(_kernel, side, heads),
            in_specs=[hbm] * 6,
            out_specs=[vmem, vmem, vmem],
            out_shape=[jax.ShapeDtypeStruct((own, cols), bf16), jax.ShapeDtypeStruct((own, d), bf16), jax.ShapeDtypeStruct(wo.shape, bf16)],
            scratch_shapes=[
                pltpu.VMEM((own, d), bf16),
                pltpu.VMEM(wq.shape, bf16),
                pltpu.VMEM((d, 2 * HEAD), bf16),
                pltpu.VMEM((HEAD, cols), bf16),
                pltpu.VMEM((n, 2, own, HEAD), bf16),
                pltpu.VMEM((HEAD + 8, cols), f32),
                pltpu.VMEM((1, cols), f32),
                pltpu.VMEM((2 * own, cols), f32),
                pltpu.VMEM((2 * own, cols), f32),
                pltpu.VMEM((2, cols), f32),
                pltpu.VMEM((2, cols), f32),
                pltpu.VMEM((own, HEAD // 2), f32),
                pltpu.VMEM((own, HEAD // 2), f32),
                pltpu.VMEM((d,), bf16),
                pltpu.SemaphoreType.DMA((12,)),
                pltpu.SemaphoreType.DMA((3,)),
                pltpu.SemaphoreType.DMA((n, 2)),
            ],
            cost_estimate=pl.CostEstimate(flops=4 * cols * n * own * HEAD, bytes_accessed=2 * wq.size, transcendentals=0),
            compiler_params=pltpu.CompilerParams(collective_id=0, has_side_effects=True, vmem_limit_bytes=VMEM),
        )(x_h, gain_h, wq_h, wk_h, wv_h, wo_h)
        return pl.pallas_call(
            _finish,
            in_specs=[vmem, vmem, vmem],
            out_specs=hbm,
            out_shape=jax.ShapeDtypeStruct((own, d), bf16),
            scratch_shapes=[pltpu.VMEM((own, d), bf16), pltpu.SemaphoreType.DMA((d // WIDE,))],
            compiler_params=pltpu.CompilerParams(vmem_limit_bytes=16 * 2**20),
            cost_estimate=pl.CostEstimate(flops=2 * own * d * cols, bytes_accessed=2 * own * d, transcendentals=0),
        )(attended, x_in, wo_in)

    tokens, whole = P(("dp", "sp"), None), P(None, None)
    return jax.shard_map(step, mesh=mesh, in_specs=(tokens, P(None), whole, whole, whole, whole), out_specs=tokens, check_vma=False)
```

```python
import functools
import math

import jax
import jax.numpy as jnp
import numpy as np
from jax import lax
from jax.experimental import pallas as pl
from jax.experimental.pallas import tpu as pltpu
from jax.sharding import PartitionSpec as P

HEAD = 256
THETA = 10000
NEG = -1e30
HIDDEN = 2 * NEG
LOG2E = 1.4426950408889634
MESH = pl.DeviceIdType.MESH
VMEM = 38 * 2**20
STRIP = 512
WIDE = 512

ORDER = ((0, 0), (-1, 0), (1, 0), (0, -1), (0, 1), (2, 0), (-1, -1), (-1, 1), (1, -1), (1, 1), (0, 2), (2, -1), (2, 1), (-1, 2), (1, 2), (2, 2))
CHIPS = ((0, 0), (-1, 0), (0, -1), (1, 0), (0, 1), (-1, -1), (-1, 1), (1, -1), (1, 1), (2, 0), (0, 2), (2, -1), (-1, 2), (2, 1), (1, 2), (2, 2))
TAKEN = {2: (6,), 3: (7, 5), 4: (8,), 5: (9,), 6: (10,), 8: (11, 12), 9: (13,), 11: (14,), 12: (15,)}
SENT = {5: (0,), 7: (1, 2), 8: (3, 4), 10: (5, 6, 7), 12: (8, 9, 10), 14: (11, 12, 13, 14)}


def _dot(a, b, ca=1, cb=0):
    return lax.dot_general(a, b, (((ca,), (cb,)), ((), ())), preferred_element_type=jnp.float32)


def _rope(t, cos, sin):
    half = t.shape[-1] // 2
    t = t.astype(jnp.bfloat16).astype(jnp.float32)
    a, b = t[:, :half], t[:, half:]
    return jnp.concatenate([a * cos - b * sin, b * cos + a * sin], -1)


def _kernel(side, heads, x_hbm, gain_hbm, wq_hbm, wk_hbm, wv_hbm, wo_hbm, out_ref, x_v, wo_v,
            a_v, wq_v, wkv_v, q_v, blk, acc, top_s, s_a, s_b, m_a, m_b, cos_v, sin_v, gain_v,
            in_sem, ssem, rsem):
    own, d = x_v.shape
    cols = heads * own
    e = HEAD**-0.5 * LOG2E
    me = lax.axis_index("sp")
    core = lax.rem(me, 2)
    chip = lax.div(me, 2)
    cx, cy = lax.div(chip, side), lax.rem(chip, side)
    p = cx + (cy - cx) * core
    s = cy + (cx - cy) * core
    wide = 2 * side
    wp, ws = wide - (wide - 2) * core, 2 + (wide - 2) * core
    partner = me + 1 - 2 * core

    def at(a, b):
        return lax.rem(p + side + a, side) * wp + lax.rem(s + side + b, side) * ws + core

    def chip_at(x, y):
        return lax.rem(cx + side + x, side) * side + lax.rem(cy + side + y, side)

    def chip_of(k):
        if isinstance(k, int):
            return chip_at(*CHIPS[k])
        bits = (side - 1).bit_length()
        x, y = (np.array([sum((c[n] % side) << bits * i for i, c in enumerate(CHIPS))]).astype(np.uint32).view(np.int32)[0].item() for n in (0, 1))
        digit = lambda packed: lax.shift_right_logical(jnp.int32(packed), jnp.int32(bits) * k) & (side - 1)
        return chip_at(digit(x), digit(y))

    right_p, left_p, right_s, left_s = at(1, 0), at(-1, 0), at(0, 1), at(0, -1)

    load_x = pltpu.make_async_copy(x_hbm, x_v, in_sem.at[0])
    load_k = pltpu.make_async_copy(wk_hbm, wkv_v.at[:, pl.ds(0, HEAD)], in_sem.at[1])
    load_v = pltpu.make_async_copy(wv_hbm, wkv_v.at[:, pl.ds(HEAD, HEAD)], in_sem.at[2])

    load_o = pltpu.make_async_copy(wo_hbm, wo_v, in_sem.at[3])

    def load_q(n):
        here = pl.ds(n * WIDE if isinstance(n, int) else pl.multiple_of(n * WIDE, WIDE), WIDE)
        return pltpu.make_async_copy(wq_hbm.at[:, here], wq_v.at[:, here], in_sem.at[4 + n])

    load_g = pltpu.make_async_copy(gain_hbm, gain_v, in_sem.at[11])
    load_x.start()
    load_g.start()
    load_k.start()
    load_v.start()
    barrier = pltpu.get_barrier_semaphore()
    for other in (right_p, left_p, right_s, left_s, partner):
        pl.semaphore_signal(barrier, inc=1, device_id={"sp": other}, device_id_type=MESH)

    place = (me * own + lax.broadcasted_iota(jnp.int32, (own, HEAD // 2), 0)).astype(jnp.float32)
    half = HEAD // 2
    angle = place * jnp.exp2(lax.broadcasted_iota(jnp.int32, (1, half), 1).astype(jnp.float32) * (-math.log2(THETA) / half))
    cos_v[...] = jnp.cos(angle)
    sin_v[...] = jnp.sin(angle)

    load_x.wait()
    load_g.wait()
    for n in range(cols // WIDE):
        load_q(n).start()
    x = x_v[...].astype(jnp.float32)
    scale = lax.rsqrt(jnp.mean(x * x, -1, keepdims=True) + 1e-6)
    a_v[...] = (x * scale * gain_v[...].astype(jnp.float32)[None]).astype(jnp.bfloat16)
    load_k.wait()
    load_v.wait()
    kv = _dot(a_v[...], wkv_v[...])
    blk[me, 0] = _rope(kv[:, :HEAD], cos_v[...], sin_v[...]).astype(jnp.bfloat16)
    blk[me, 1] = kv[:, HEAD:].T.astype(jnp.bfloat16)

    def line_end(n):
        return lax.rem(p + side + n, side) * (side - (side - 1) * core) + (side - 1) * (1 + (side - 1) * core)

    def along(n):
        return lax.div(at(0, n), 2)

    def arrives(k):
        (a, b), of = ORDER[k], lax.div(at(*ORDER[k]), 2)
        if b == 0:
            return line_end(0) > of if a == 2 else (line_end(0) > of) | (line_end(-a) > of)
        return along(0) > of if b == 2 else (along(0) > of) | (along(-b) > of)

    def sends_of(k):
        (a, b), of = ORDER[k], lax.div(at(*ORDER[k]), 2)
        out = [(along(0) > of if k else None, None, partner)]
        if b == 0:
            out += [((along(n) > of) | (along(2) > of), None, at(0, n)) for n in (1, -1)]
        elif b != 2:
            out += [(along(-b) > of, 0 if b < 0 else 1, at(0, -b))]
        if k == 0:
            out += [((line_end(n) > of) | (line_end(2) > of), None, at(n, 0)) for n in (1, -1)]
        elif b == 0 and a != 2:
            out += [(line_end(-a) > of, 0 if a < 0 else 1, at(-a, 0))]
        return out

    def copy_of(block, part, other, send=0):
        ref = blk.at[block] if part is None else blk.at[block, part]
        return pltpu.make_async_remote_copy(src_ref=ref, dst_ref=ref, send_sem=ssem.at[send], recv_sem=rsem.at[block, part or 0],
                                            device_id={"sp": other}, device_id_type=MESH)

    def send(k, which):
        block, todo = at(*ORDER[k]), sends_of(k)
        for n in which if which else range(len(todo)):
            whether, part, other = todo[n]
            copy = copy_of(block, part, other, 5 * k + n)
            copy.start() if whether is None else pl.when(whether)(copy.start)

    def sent(k):
        for n, (whether, part, other) in enumerate(sends_of(k)):
            copy = copy_of(me, part, other, 5 * k + n)
            copy.wait_send() if whether is None else pl.when(whether)(copy.wait_send)

    def arrived(block):
        copy_of(block, None, partner).wait_recv()

    pl.semaphore_wait(barrier, 5)
    send(0, (3, 4, 0))

    def project(n, _):
        load_q(n).wait()
        here = pl.ds(pl.multiple_of(n * WIDE, WIDE), WIDE)
        q = _dot(a_v[...], wq_v[:, here])
        for h in range(WIDE // HEAD):
            turned = _rope(q[:, h * HEAD : (h + 1) * HEAD], cos_v[...], sin_v[...])
            q_v[:, pl.ds(pl.multiple_of(n * WIDE + h * HEAD, HEAD), HEAD)] = turned.T.astype(jnp.bfloat16)
        return _

    lax.fori_loop(0, cols // WIDE - 1, project, None)
    load_o.start()
    send(0, (1, 2))
    lax.fori_loop(cols // WIDE - 1, cols // WIDE, project, None)

    def exchange(k):
        a, b = ORDER[k]
        block = at(a, b)

        @pl.when(arrives(k))
        def _():
            if b == 2 or (a, b) == (2, 0):
                copy_of(block, 0, partner).wait_recv()
                copy_of(block, 1, partner).wait_recv()
            else:
                arrived(block)

        if k in (1, 2):
            send(k, (1, 2, 0))
        else:
            send(k, None)
        if k == 4:
            send(1, (3,))
            send(2, (3,))

    strips = range(0, cols, STRIP)

    def scores(k, out, most):
        chip = chip_of(k)
        for n in (0, 1):
            for c in strips:
                sc = _dot(blk[2 * chip + n, 0], q_v[:, c : c + STRIP]) * e
                out[n * own : (n + 1) * own, c : c + STRIP] = sc
                most[n : n + 1, c : c + STRIP] = sc.max(axis=0, keepdims=True)

    def attend(k, sc, most):
        chip = chip_of(k)
        values = jnp.concatenate([blk[2 * chip, 1], blk[2 * chip + 1, 1]], axis=1)
        values = jnp.concatenate([values, jnp.ones((8, 2 * own), jnp.bfloat16)], axis=0)
        first_step = isinstance(k, int) and k == 0
        for c in strips:
            here = slice(c, c + STRIP)
            weights = sc[:, here]
            if first_step:
                query = core * own + lax.rem(lax.broadcasted_iota(jnp.int32, (2 * own, STRIP), 1), own)
                weights = jnp.where(query >= lax.broadcasted_iota(jnp.int32, (2 * own, STRIP), 0), weights, HIDDEN)
                top = weights.max(axis=0, keepdims=True)
            else:
                old = top_s[:, here]
                top = jnp.maximum(old, jnp.maximum(most[:1, here], most[1:2, here]))
                keep = jnp.exp2(old - top)
            top_s[:, here] = top
            got = _dot(values, jnp.exp2(weights - top).astype(jnp.bfloat16))
            acc[:, here] = got if first_step else acc[:, here] * keep + got

    last = len(CHIPS) - 1

    def other_block(k):
        return 2 * chip_of(k) + 1 - core

    arrived(partner)
    scores(0, s_a, m_a)
    exchange(1)
    exchange(2)
    attend(0, s_a, m_a)
    exchange(3)
    exchange(4)
    pl.when(chip_of(1) < chip)(lambda: arrived(other_block(1)))
    scores(1, s_b, m_b)

    def pair(t, _):
        for odd in (0, 1):
            k = 1 + odd + 2 * t
            for n, taken in TAKEN.items():
                if n % 2 != odd:
                    @pl.when(k == n)
                    def _():
                        for r in taken:
                            exchange(r)

            for n, done in SENT.items():
                if n % 2 != odd:
                    @pl.when(k == n)
                    def _():
                        for r in done:
                            sent(r)

            ahead = chip_of(k + 1) < chip
            pl.when(ahead)(lambda: arrived(other_block(k + 1)))
            now, later = ((s_a, m_a), (s_b, m_b)) if odd else ((s_b, m_b), (s_a, m_a))
            seen = chip_of(k) < chip

            @pl.when(seen)
            def _():
                scores(k + 1, *later)
                attend(k, *now)

            @pl.when(ahead & ~seen)
            def _():
                scores(k + 1, *later)

        return _

    lax.fori_loop(0, (last - 1) // 2, pair, None)
    pl.when(chip_of(last) < chip)(functools.partial(attend, last, s_b, m_b))

    for h in range(heads):
        here = slice(h * own, (h + 1) * own)
        out = acc[:HEAD, here] * (1 / acc[HEAD : HEAD + 1, here])
        out_ref[:, h * HEAD : (h + 1) * HEAD] = out.T.astype(jnp.bfloat16)

    load_o.wait()
    for k in range(len(ORDER)):
        if all(k not in done for done in SENT.values()):
            sent(k)


def _finish(a_ref, x_ref, wo_ref, y_hbm, y_v, out_sem):
    def result(n):
        here = pl.ds(n * WIDE, WIDE)
        return pltpu.make_async_copy(y_v.at[:, here], y_hbm.at[:, here], out_sem.at[n])

    chunks = range(x_ref.shape[1] // WIDE)
    for n in chunks:
        here = slice(n * WIDE, (n + 1) * WIDE)
        y_v[:, here] = (x_ref[:, here].astype(jnp.float32) + _dot(a_ref[...], wo_ref[:, here])).astype(jnp.bfloat16)
        result(n).start()
    for n in chunks:
        result(n).wait()


def solution(mesh):
    side = math.isqrt(mesh.shape["sp"] // 2)

    def step(x, gain, wq, wk, wv, wo):
        own, d = x.shape
        heads = wq.shape[1] // HEAD
        cols = heads * own
        n = mesh.shape["sp"]
        hbm, vmem = pl.BlockSpec(memory_space=pltpu.HBM), pl.BlockSpec(memory_space=pltpu.VMEM)
        bf16, f32 = jnp.bfloat16, jnp.float32
        x_h, wq_h, wk_h, wv_h, wo_h = (pltpu.with_memory_space_constraint(t, pltpu.HBM) for t in (x, wq, wk, wv, wo))
        gain_h = pltpu.with_memory_space_constraint(gain, pltpu.HBM)
        attended, x_in, wo_in = pl.pallas_call(
            functools.partial(_kernel, side, heads),
            in_specs=[hbm] * 6,
            out_specs=[vmem, vmem, vmem],
            out_shape=[jax.ShapeDtypeStruct((own, cols), bf16), jax.ShapeDtypeStruct((own, d), bf16), jax.ShapeDtypeStruct(wo.shape, bf16)],
            scratch_shapes=[
                pltpu.VMEM((own, d), bf16),
                pltpu.VMEM(wq.shape, bf16),
                pltpu.VMEM((d, 2 * HEAD), bf16),
                pltpu.VMEM((HEAD, cols), bf16),
                pltpu.VMEM((n, 2, own, HEAD), bf16),
                pltpu.VMEM((HEAD + 8, cols), f32),
                pltpu.VMEM((1, cols), f32),
                pltpu.VMEM((2 * own, cols), f32),
                pltpu.VMEM((2 * own, cols), f32),
                pltpu.VMEM((2, cols), f32),
                pltpu.VMEM((2, cols), f32),
                pltpu.VMEM((own, HEAD // 2), f32),
                pltpu.VMEM((own, HEAD // 2), f32),
                pltpu.VMEM((d,), bf16),
                pltpu.SemaphoreType.DMA((12,)),
                pltpu.SemaphoreType.DMA((5 * len(ORDER),)),
                pltpu.SemaphoreType.DMA((n, 2)),
            ],
            cost_estimate=pl.CostEstimate(flops=4 * cols * n * own * HEAD, bytes_accessed=2 * wq.size, transcendentals=0),
            compiler_params=pltpu.CompilerParams(collective_id=0, has_side_effects=True, vmem_limit_bytes=VMEM),
        )(x_h, gain_h, wq_h, wk_h, wv_h, wo_h)
        return pl.pallas_call(
            _finish,
            in_specs=[vmem, vmem, vmem],
            out_specs=hbm,
            out_shape=jax.ShapeDtypeStruct((own, d), bf16),
            scratch_shapes=[pltpu.VMEM((own, d), bf16), pltpu.SemaphoreType.DMA((d // WIDE,))],
            compiler_params=pltpu.CompilerParams(vmem_limit_bytes=16 * 2**20),
            cost_estimate=pl.CostEstimate(flops=2 * own * d * cols, bytes_accessed=2 * own * d, transcendentals=0),
        )(attended, x_in, wo_in)

    tokens, whole = P(("dp", "sp"), None), P(None, None)
    return jax.shard_map(step, mesh=mesh, in_specs=(tokens, P(None), whole, whole, whole, whole), out_specs=tokens, check_vma=False)
```

```python
import functools
import math

import jax
import jax.numpy as jnp
import numpy as np
from jax import lax
from jax.experimental import pallas as pl
from jax.experimental.pallas import tpu as pltpu
from jax.sharding import PartitionSpec as P

HEAD = 256
THETA = 10000
NEG = -1e30
HIDDEN = 2 * NEG
LOG2E = 1.4426950408889634
MESH = pl.DeviceIdType.MESH
VMEM = 38 * 2**20
STRIP = 512
WIDE = 512

ORDER = ((0, 0), (-1, 0), (1, 0), (0, -1), (0, 1), (2, 0), (-1, -1), (-1, 1), (1, -1), (1, 1), (0, 2), (2, -1), (2, 1), (-1, 2), (1, 2), (2, 2))
CHIPS = ((0, 0), (-1, 0), (0, -1), (1, 0), (0, 1), (-1, -1), (-1, 1), (1, -1), (1, 1), (2, 0), (0, 2), (2, -1), (-1, 2), (2, 1), (1, 2), (2, 2))
TAKEN = {2: (6,), 3: (7, 5), 4: (8,), 5: (9,), 6: (10,), 8: (11, 12), 9: (13,), 11: (14,), 12: (15,)}
SENT = {5: (0,), 7: (1, 2), 8: (3, 4), 10: (5, 6, 7), 12: (8, 9, 10), 14: (11, 12, 13, 14)}


RANK = {(a % 4, b % 4): k for k, (a, b) in enumerate(ORDER)}
STEP = {(x % 4, y % 4): k for k, (x, y) in enumerate(CHIPS)}
HALVED = (5, 10, 13, 14, 15)
BASE = (0, 5, 9, 13, 15, 17, 20, 22, 24, 26, 0, 5, 9, 13, 15, 17)


def _landing(k, half):
    return k - 1 if half != 1 else len(ORDER) - 1 + HALVED.index(k)


def _dot(a, b, ca=1, cb=0):
    return lax.dot_general(a, b, (((ca,), (cb,)), ((), ())), preferred_element_type=jnp.float32)


def _rope(t, cos, sin):
    half = t.shape[-1] // 2
    t = t.astype(jnp.bfloat16).astype(jnp.float32)
    a, b = t[:, :half], t[:, half:]
    return jnp.concatenate([a * cos - b * sin, b * cos + a * sin], -1)


def _kernel(side, heads, x_hbm, gain_hbm, wq_hbm, wk_hbm, wv_hbm, wo_hbm, out_ref, x_v, wo_v,
            a_v, wq_v, wkv_v, q_v, blk, acc, top_s, s_a, s_b, m_a, m_b, cos_v, sin_v, gain_v,
            in_sem, ssem, rsem):
    own, d = x_v.shape
    cols = heads * own
    e = HEAD**-0.5 * LOG2E
    me = lax.axis_index("sp")
    around = side - 1
    bits = around.bit_length()
    core = me & 1
    chip = me >> 1
    cx, cy = chip >> bits, chip & around
    p = cx + (cy - cx) * core
    s = cy + (cx - cy) * core
    wide = 2 * side
    wp, ws = wide - (wide - 2) * core, 2 + (wide - 2) * core
    partner = me + 1 - 2 * core

    def at(a, b):
        return ((p + a) & around) * wp + ((s + b) & around) * ws + core

    def chip_at(x, y):
        return (((cx + x) & around) << bits) + ((cy + y) & around)

    def chip_of(k):
        if isinstance(k, int):
            return chip_at(*CHIPS[k])
        x, y = (np.array([sum((c[n] % side) << bits * i for i, c in enumerate(CHIPS))]).astype(np.uint32).view(np.int32)[0].item() for n in (0, 1))
        digit = lambda packed: lax.shift_right_logical(jnp.int32(packed), jnp.int32(bits) * k) & around
        return chip_at(digit(x), digit(y))

    right_p, left_p, right_s, left_s = at(1, 0), at(-1, 0), at(0, 1), at(0, -1)

    load_x = pltpu.make_async_copy(x_hbm, x_v, in_sem.at[0])
    load_k = pltpu.make_async_copy(wk_hbm, wkv_v.at[:, pl.ds(0, HEAD)], in_sem.at[1])
    load_v = pltpu.make_async_copy(wv_hbm, wkv_v.at[:, pl.ds(HEAD, HEAD)], in_sem.at[2])

    load_o = pltpu.make_async_copy(wo_hbm, wo_v, in_sem.at[3])

    def load_q(n):
        here = pl.ds(n * WIDE if isinstance(n, int) else pl.multiple_of(n * WIDE, WIDE), WIDE)
        return pltpu.make_async_copy(wq_hbm.at[:, here], wq_v.at[:, here], in_sem.at[4 + n])

    load_g = pltpu.make_async_copy(gain_hbm, gain_v, in_sem.at[8])
    load_x.start()
    load_g.start()
    load_k.start()
    load_v.start()
    barrier = pltpu.get_barrier_semaphore()
    for other in (right_p, left_p, right_s, left_s, partner):
        pl.semaphore_signal(barrier, inc=1, device_id={"sp": other}, device_id_type=MESH)

    place = (me * own + lax.broadcasted_iota(jnp.int32, (own, HEAD // 2), 0)).astype(jnp.float32)
    half = HEAD // 2
    angle = place * jnp.exp2(lax.broadcasted_iota(jnp.int32, (1, half), 1).astype(jnp.float32) * (-math.log2(THETA) / half))
    cos_v[...] = jnp.cos(angle)
    sin_v[...] = jnp.sin(angle)

    load_x.wait()
    load_g.wait()
    for n in range(cols // WIDE):
        load_q(n).start()
    x = x_v[...].astype(jnp.float32)
    scale = lax.rsqrt(jnp.mean(x * x, -1, keepdims=True) + 1e-6)
    a_v[...] = (x * scale * gain_v[...].astype(jnp.float32)[None]).astype(jnp.bfloat16)
    load_k.wait()
    load_v.wait()
    kv = _dot(a_v[...], wkv_v[...])
    blk[me, 0] = _rope(kv[:, :HEAD], cos_v[...], sin_v[...]).astype(jnp.bfloat16)
    blk[me, 1] = kv[:, HEAD:].T.astype(jnp.bfloat16)

    def line_end(n):
        return ((p + n) & around) * (side - around * core) + around * (1 + around * core)

    def along(n):
        return at(0, n) >> 1

    def arrives(k):
        (a, b), of = ORDER[k], at(*ORDER[k]) >> 1
        if b == 0:
            return line_end(0) > of if a == 2 else (line_end(0) > of) | (line_end(-a) > of)
        return along(0) > of if b == 2 else (along(0) > of) | (along(-b) > of)

    def sends_of(k):
        (a, b), of = ORDER[k], at(*ORDER[k]) >> 1
        x, y = STEP[a % 4, b % 4], STEP[b % 4, a % 4]
        out = [(along(0) > of if k else None, None, partner, 20 + x + (y - x) * core)]
        if b == 0:
            out += [((along(n) > of) | (along(2) > of), None, at(0, n), _landing(RANK[a % 4, (b - n) % 4], None)) for n in (1, -1)]
        elif b != 2:
            half = 0 if b < 0 else 1
            out += [(along(-b) > of, half, at(0, -b), _landing(RANK[a % 4, 2], half))]
        if k == 0:
            out += [((line_end(n) > of) | (line_end(2) > of), None, at(n, 0), _landing(RANK[-n % 4, 0], None)) for n in (1, -1)]
        elif b == 0 and a != 2:
            half = 0 if a < 0 else 1
            out += [(line_end(-a) > of, half, at(-a, 0), _landing(RANK[2, 0], half))]
        return out

    def copy_of(block, part, other, send, landing):
        ref = blk.at[block] if part is None else blk.at[block, part]
        return pltpu.make_async_remote_copy(src_ref=ref, dst_ref=ref, send_sem=ssem.at[send], recv_sem=rsem.at[landing],
                                            device_id={"sp": other}, device_id_type=MESH)

    def send(k, which):
        block, todo = at(*ORDER[k]), sends_of(k)
        for n in which if which else range(len(todo)):
            whether, part, other, landing = todo[n]
            copy = copy_of(block, part, other, BASE[k] + n, landing)
            copy.start() if whether is None else pl.when(whether)(copy.start)

    def sent(k):
        for n, (whether, part, other, landing) in enumerate(sends_of(k)):
            copy = copy_of(me, part, other, BASE[k] + n, landing)
            copy.wait_send() if whether is None else pl.when(whether)(copy.wait_send)

    def arrived(block, landing, part=None):
        copy_of(block, part, partner, 0, landing).wait_recv()

    pl.semaphore_wait(barrier, 5)
    send(0, (3, 4))

    def project(n, _):
        load_q(n).wait()
        here = pl.ds(pl.multiple_of(n * WIDE, WIDE), WIDE)
        q = _dot(a_v[...], wq_v[:, here])
        for h in range(WIDE // HEAD):
            turned = _rope(q[:, h * HEAD : (h + 1) * HEAD], cos_v[...], sin_v[...])
            q_v[:, pl.ds(pl.multiple_of(n * WIDE + h * HEAD, HEAD), HEAD)] = turned.T.astype(jnp.bfloat16)
        return _

    lax.fori_loop(0, 1, project, None)
    send(0, (0,))
    lax.fori_loop(1, cols // WIDE - 1, project, None)
    load_o.start()
    send(0, (1, 2))
    lax.fori_loop(cols // WIDE - 1, cols // WIDE, project, None)

    def exchange(k):
        a, b = ORDER[k]
        block = at(a, b)

        @pl.when(arrives(k))
        def _():
            for half in (0, 1) if k in HALVED else (None,):
                arrived(block, _landing(k, half), half)

        if k in (1, 2):
            send(k, (1, 2, 0))
        else:
            send(k, None)
        if k == 4:
            send(1, (3,))
            send(2, (3,))

    strips = range(0, cols, STRIP)
    last = len(CHIPS) - 1

    def scores(k, out, most):
        chip = chip_of(k)
        for n in (0, 1):
            for c in strips:
                sc = _dot(blk[2 * chip + n, 0], q_v[:, c : c + STRIP]) * e
                out[n * own : (n + 1) * own, c : c + STRIP] = sc
                most[n : n + 1, c : c + STRIP] = sc.max(axis=0, keepdims=True)

    def attend(k, sc, most):
        chip = chip_of(k)
        values = jnp.concatenate([blk[2 * chip, 1], blk[2 * chip + 1, 1]], axis=1)
        values = jnp.concatenate([values, jnp.ones((8, 2 * own), jnp.bfloat16)], axis=0)
        first_step = isinstance(k, int) and k == 0
        for c in strips:
            here = slice(c, c + STRIP)
            weights = sc[:, here]
            if first_step:
                query = core * own + lax.rem(lax.broadcasted_iota(jnp.int32, (2 * own, STRIP), 1), own)
                weights = jnp.where(query >= lax.broadcasted_iota(jnp.int32, (2 * own, STRIP), 0), weights, HIDDEN)
                top = weights.max(axis=0, keepdims=True)
            else:
                old = top_s[:, here]
                top = jnp.maximum(old, jnp.maximum(most[:1, here], most[1:2, here]))
                keep = jnp.exp2(old - top)
            top_s[:, here] = top
            got = _dot(values, jnp.exp2(weights - top).astype(jnp.bfloat16))
            total = got if first_step else acc[:, here] * keep + got
            if k == last if isinstance(k, int) else False:
                finish(total, c)
            else:
                acc[:, here] = total

    def finish(total, c):
        for h in range(STRIP // own):
            of = slice(h * own, (h + 1) * own)
            out = total[:HEAD, of] * (1 / total[HEAD : HEAD + 1, of])
            at_head = (c // own + h) * HEAD
            out_ref[:, at_head : at_head + HEAD] = out.T.astype(jnp.bfloat16)


    def other_block(k):
        return 2 * chip_of(k) + 1 - core

    arrived(partner, 20)
    scores(0, s_a, m_a)
    exchange(1)
    exchange(2)
    attend(0, s_a, m_a)
    exchange(3)
    exchange(4)
    pl.when(chip_of(1) < chip)(lambda: arrived(other_block(1), 21))
    scores(1, s_b, m_b)

    def pair(t, _):
        for odd in (0, 1):
            k = 1 + odd + 2 * t
            for n, taken in TAKEN.items():
                if n % 2 != odd:
                    @pl.when(k == n)
                    def _():
                        for r in taken:
                            exchange(r)

            for n, done in SENT.items():
                if n % 2 != odd:
                    @pl.when(k == n)
                    def _():
                        for r in done:
                            sent(r)

            ahead = chip_of(k + 1) < chip
            pl.when(ahead)(lambda: arrived(other_block(k + 1), 21 + k))
            now, later = ((s_a, m_a), (s_b, m_b)) if odd else ((s_b, m_b), (s_a, m_a))
            seen = chip_of(k) < chip

            @pl.when(seen)
            def _():
                scores(k + 1, *later)
                attend(k, *now)

            @pl.when(ahead & ~seen)
            def _():
                scores(k + 1, *later)

        return _

    lax.fori_loop(0, (last - 1) // 2, pair, None)
    pl.when(chip_of(last) < chip)(functools.partial(attend, last, s_b, m_b))

    @pl.when(chip_of(last) >= chip)
    def _():
        for c in strips:
            finish(acc[:, c : c + STRIP], c)

    load_o.wait()
    for k in range(len(ORDER)):
        if all(k not in done for done in SENT.values()):
            sent(k)


def _finish(a_ref, x_ref, wo_ref, y_hbm, y_v, out_sem):
    def result(n):
        here = pl.ds(n * WIDE, WIDE)
        return pltpu.make_async_copy(y_v.at[:, here], y_hbm.at[:, here], out_sem.at[n])

    chunks = range(x_ref.shape[1] // WIDE)
    for n in chunks:
        here = slice(n * WIDE, (n + 1) * WIDE)
        y_v[:, here] = (x_ref[:, here].astype(jnp.float32) + _dot(a_ref[...], wo_ref[:, here])).astype(jnp.bfloat16)
        result(n).start()
    for n in chunks:
        result(n).wait()


def solution(mesh):
    side = math.isqrt(mesh.shape["sp"] // 2)
    assert 2 * side * side == mesh.shape["sp"] and side == 4

    def step(x, gain, wq, wk, wv, wo):
        own, d = x.shape
        heads = wq.shape[1] // HEAD
        cols = heads * own
        n = mesh.shape["sp"]
        hbm, vmem = pl.BlockSpec(memory_space=pltpu.HBM), pl.BlockSpec(memory_space=pltpu.VMEM)
        bf16, f32 = jnp.bfloat16, jnp.float32
        x_h, wq_h, wk_h, wv_h, wo_h = (pltpu.with_memory_space_constraint(t, pltpu.HBM) for t in (x, wq, wk, wv, wo))
        gain_h = pltpu.with_memory_space_constraint(gain, pltpu.HBM)
        attended, x_in, wo_in = pl.pallas_call(
            functools.partial(_kernel, side, heads),
            in_specs=[hbm] * 6,
            out_specs=[vmem, vmem, vmem],
            out_shape=[jax.ShapeDtypeStruct((own, cols), bf16), jax.ShapeDtypeStruct((own, d), bf16), jax.ShapeDtypeStruct(wo.shape, bf16)],
            scratch_shapes=[
                pltpu.VMEM((own, d), bf16),
                pltpu.VMEM(wq.shape, bf16),
                pltpu.VMEM((d, 2 * HEAD), bf16),
                pltpu.VMEM((HEAD, cols), bf16),
                pltpu.VMEM((n, 2, own, HEAD), bf16),
                pltpu.VMEM((HEAD + 8, cols), f32),
                pltpu.VMEM((1, cols), f32),
                pltpu.VMEM((2 * own, cols), f32),
                pltpu.VMEM((2 * own, cols), f32),
                pltpu.VMEM((2, cols), f32),
                pltpu.VMEM((2, cols), f32),
                pltpu.VMEM((own, HEAD // 2), f32),
                pltpu.VMEM((own, HEAD // 2), f32),
                pltpu.VMEM((d,), bf16),
                pltpu.SemaphoreType.DMA((9,)),
                pltpu.SemaphoreType.DMA((28,)),
                pltpu.SemaphoreType.DMA((20 + len(CHIPS),)),
            ],
            cost_estimate=pl.CostEstimate(flops=4 * cols * n * own * HEAD, bytes_accessed=2 * wq.size, transcendentals=0),
            compiler_params=pltpu.CompilerParams(collective_id=0, has_side_effects=True, vmem_limit_bytes=VMEM),
        )(x_h, gain_h, wq_h, wk_h, wv_h, wo_h)
        return pl.pallas_call(
            _finish,
            in_specs=[vmem, vmem, vmem],
            out_specs=hbm,
            out_shape=jax.ShapeDtypeStruct((own, d), bf16),
            scratch_shapes=[pltpu.VMEM((own, d), bf16), pltpu.SemaphoreType.DMA((d // WIDE,))],
            compiler_params=pltpu.CompilerParams(vmem_limit_bytes=16 * 2**20),
            cost_estimate=pl.CostEstimate(flops=2 * own * d * cols, bytes_accessed=2 * own * d, transcendentals=0),
        )(attended, x_in, wo_in)

    tokens, whole = P(("dp", "sp"), None), P(None, None)
    return jax.shard_map(step, mesh=mesh, in_specs=(tokens, P(None), whole, whole, whole, whole), out_specs=tokens, check_vma=False)
```

```python
import functools
import math

import jax
import jax.numpy as jnp
import numpy as np
from jax import lax
from jax.experimental import pallas as pl
from jax.experimental.pallas import tpu as pltpu
from jax.sharding import PartitionSpec as P

HEAD = 256
THETA = 10000
NEG = -1e30
HIDDEN = 2 * NEG
LOG2E = 1.4426950408889634
MESH = pl.DeviceIdType.MESH
VMEM = 38 * 2**20
STRIP = 512
WIDE = 512

ORDER = ((0, 0), (-1, 0), (1, 0), (0, -1), (0, 1), (2, 0), (-1, -1), (-1, 1), (1, -1), (1, 1), (0, 2), (2, -1), (2, 1), (-1, 2), (1, 2), (2, 2))
CHIPS = ((0, 0), (-1, 0), (0, -1), (1, 0), (0, 1), (-1, -1), (-1, 1), (1, -1), (1, 1), (2, 0), (0, 2), (2, -1), (-1, 2), (2, 1), (1, 2), (2, 2))
TAKEN = {2: (6,), 3: (7, 5), 4: (8,), 5: (9,), 6: (10,), 8: (11,), 9: (12, 13), 11: (14,), 12: (15,)}
SENT = {5: (0,), 7: (1, 2, 3, 4), 10: (5, 6, 7), 12: (8, 9, 10), 13: (11, 12, 13, 14)}
SINGLE = 12


RANK = {(a % 4, b % 4): k for k, (a, b) in enumerate(ORDER)}
STEP = {(x % 4, y % 4): k for k, (x, y) in enumerate(CHIPS)}
HALVED = (5, 10, 13, 14, 15)
BASE = (0, 5, 9, 13, 15, 17, 20, 22, 24, 26, 0, 5, 9, 13, 15, 17)


def _landing(k, half):
    return k - 1 if half != 1 else len(ORDER) - 1 + HALVED.index(k)


def _dot(a, b, ca=1, cb=0):
    return lax.dot_general(a, b, (((ca,), (cb,)), ((), ())), preferred_element_type=jnp.float32)


def _rope(t, cos, sin):
    half = t.shape[-1] // 2
    t = t.astype(jnp.bfloat16).astype(jnp.float32)
    a, b = t[:, :half], t[:, half:]
    return jnp.concatenate([a * cos - b * sin, b * cos + a * sin], -1)


def _kernel(side, heads, x_hbm, gain_hbm, wq_hbm, wk_hbm, wv_hbm, wo_hbm, out_ref, x_v, wo_v,
            a_v, wq_v, wkv_v, q_v, blk, acc, top_s, s_a, s_b, m_a, m_b, cos_v, sin_v, gain_v,
            in_sem, ssem, rsem):
    own, d = x_v.shape
    cols = heads * own
    e = HEAD**-0.5 * LOG2E
    me = lax.axis_index("sp")
    around = side - 1
    bits = around.bit_length()
    core = me & 1
    chip = me >> 1
    cx, cy = chip >> bits, chip & around
    p = cx + (cy - cx) * core
    s = cy + (cx - cy) * core
    wide = 2 * side
    wp, ws = wide - (wide - 2) * core, 2 + (wide - 2) * core
    partner = me + 1 - 2 * core

    def at(a, b):
        return ((p + a) & around) * wp + ((s + b) & around) * ws + core

    def chip_at(x, y):
        return (((cx + x) & around) << bits) + ((cy + y) & around)

    def chip_of(k):
        if isinstance(k, int):
            return chip_at(*CHIPS[k])
        x, y = (np.array([sum((c[n] % side) << bits * i for i, c in enumerate(CHIPS))]).astype(np.uint32).view(np.int32)[0].item() for n in (0, 1))
        digit = lambda packed: lax.shift_right_logical(jnp.int32(packed), jnp.int32(bits) * k) & around
        return chip_at(digit(x), digit(y))

    right_p, left_p, right_s, left_s = at(1, 0), at(-1, 0), at(0, 1), at(0, -1)

    load_x = pltpu.make_async_copy(x_hbm, x_v, in_sem.at[0])
    load_k = pltpu.make_async_copy(wk_hbm, wkv_v.at[:, pl.ds(0, HEAD)], in_sem.at[1])
    load_v = pltpu.make_async_copy(wv_hbm, wkv_v.at[:, pl.ds(HEAD, HEAD)], in_sem.at[2])

    load_o = pltpu.make_async_copy(wo_hbm, wo_v, in_sem.at[3])

    def load_q(n):
        here = pl.ds(n * WIDE if isinstance(n, int) else pl.multiple_of(n * WIDE, WIDE), WIDE)
        return pltpu.make_async_copy(wq_hbm.at[:, here], wq_v.at[:, here], in_sem.at[4 + n])

    load_g = pltpu.make_async_copy(gain_hbm, gain_v, in_sem.at[8])
    load_x.start()
    load_g.start()
    load_k.start()
    load_v.start()
    barrier = pltpu.get_barrier_semaphore()
    for other in (right_p, left_p, right_s, left_s, partner):
        pl.semaphore_signal(barrier, inc=1, device_id={"sp": other}, device_id_type=MESH)

    place = (me * own + lax.broadcasted_iota(jnp.int32, (own, HEAD // 2), 0)).astype(jnp.float32)
    half = HEAD // 2
    angle = place * jnp.exp2(lax.broadcasted_iota(jnp.int32, (1, half), 1).astype(jnp.float32) * (-math.log2(THETA) / half))
    cos_v[...] = jnp.cos(angle)
    sin_v[...] = jnp.sin(angle)

    load_x.wait()
    load_g.wait()
    for n in range(cols // WIDE):
        load_q(n).start()
    x = x_v[...].astype(jnp.float32)
    scale = lax.rsqrt(jnp.mean(x * x, -1, keepdims=True) + 1e-6)
    a_v[...] = (x * scale * gain_v[...].astype(jnp.float32)[None]).astype(jnp.bfloat16)
    load_k.wait()
    load_v.wait()
    kv = _dot(a_v[...], wkv_v[...])
    blk[me, 0] = _rope(kv[:, :HEAD], cos_v[...], sin_v[...]).astype(jnp.bfloat16)
    blk[me, 1] = kv[:, HEAD:].T.astype(jnp.bfloat16)

    def line_end(n):
        return ((p + n) & around) * (side - around * core) + around * (1 + around * core)

    def along(n):
        return at(0, n) >> 1

    def arrives(k):
        (a, b), of = ORDER[k], at(*ORDER[k]) >> 1
        if b == 0:
            return line_end(0) > of if a == 2 else (line_end(0) > of) | (line_end(-a) > of)
        return along(0) > of if b == 2 else (along(0) > of) | (along(-b) > of)

    def sends_of(k):
        (a, b), of = ORDER[k], at(*ORDER[k]) >> 1
        x, y = STEP[a % 4, b % 4], STEP[b % 4, a % 4]
        out = [(along(0) > of if k else None, None, partner, 20 + x + (y - x) * core)]
        if b == 0:
            out += [((along(n) > of) | (along(2) > of), None, at(0, n), _landing(RANK[a % 4, (b - n) % 4], None)) for n in (1, -1)]
        elif b != 2:
            half = 0 if b < 0 else 1
            out += [(along(-b) > of, half, at(0, -b), _landing(RANK[a % 4, 2], half))]
        if k == 0:
            out += [((line_end(n) > of) | (line_end(2) > of), None, at(n, 0), _landing(RANK[-n % 4, 0], None)) for n in (1, -1)]
        elif b == 0 and a != 2:
            half = 0 if a < 0 else 1
            out += [(line_end(-a) > of, half, at(-a, 0), _landing(RANK[2, 0], half))]
        return out

    def copy_of(block, part, other, send, landing):
        ref = blk.at[block] if part is None else blk.at[block, part]
        return pltpu.make_async_remote_copy(src_ref=ref, dst_ref=ref, send_sem=ssem.at[send], recv_sem=rsem.at[landing],
                                            device_id={"sp": other}, device_id_type=MESH)

    def send(k, which):
        block, todo = at(*ORDER[k]), sends_of(k)
        for n in which if which else range(len(todo)):
            whether, part, other, landing = todo[n]
            copy = copy_of(block, part, other, BASE[k] + n, landing)
            copy.start() if whether is None else pl.when(whether)(copy.start)

    def sent(k):
        for n, (whether, part, other, landing) in enumerate(sends_of(k)):
            copy = copy_of(me, part, other, BASE[k] + n, landing)
            copy.wait_send() if whether is None else pl.when(whether)(copy.wait_send)

    def arrived(block, landing, part=None):
        copy_of(block, part, partner, 0, landing).wait_recv()

    pl.semaphore_wait(barrier, 5)
    send(0, (3, 4))

    def project(n, _):
        load_q(n).wait()
        here = pl.ds(pl.multiple_of(n * WIDE, WIDE), WIDE)
        q = _dot(a_v[...], wq_v[:, here])
        for h in range(WIDE // HEAD):
            turned = _rope(q[:, h * HEAD : (h + 1) * HEAD], cos_v[...], sin_v[...])
            q_v[:, pl.ds(pl.multiple_of(n * WIDE + h * HEAD, HEAD), HEAD)] = turned.T.astype(jnp.bfloat16)
        return _

    lax.fori_loop(0, 1, project, None)
    send(0, (0,))
    lax.fori_loop(1, cols // WIDE - 1, project, None)
    load_o.start()
    send(0, (1, 2))
    lax.fori_loop(cols // WIDE - 1, cols // WIDE, project, None)

    def exchange(k):
        a, b = ORDER[k]
        block = at(a, b)

        @pl.when(arrives(k))
        def _():
            for half in (0, 1) if k in HALVED else (None,):
                arrived(block, _landing(k, half), half)

        if k in (1, 2):
            send(k, (1, 2, 0))
        else:
            send(k, None)
        if k == 4:
            send(1, (3,))
            send(2, (3,))

    strips = range(0, cols, STRIP)
    last = len(CHIPS) - 1

    def scores(k, out, most):
        chip = chip_of(k)
        for n in (0, 1):
            for c in strips:
                sc = _dot(blk[2 * chip + n, 0], q_v[:, c : c + STRIP]) * e
                out[n * own : (n + 1) * own, c : c + STRIP] = sc
                most[n : n + 1, c : c + STRIP] = sc.max(axis=0, keepdims=True)

    def attend(k, sc, most):
        chip = chip_of(k)
        values = jnp.concatenate([blk[2 * chip, 1], blk[2 * chip + 1, 1]], axis=1)
        values = jnp.concatenate([values, jnp.ones((8, 2 * own), jnp.bfloat16)], axis=0)
        first_step = isinstance(k, int) and k == 0
        for c in strips:
            here = slice(c, c + STRIP)
            weights = sc[:, here]
            if first_step:
                query = core * own + lax.rem(lax.broadcasted_iota(jnp.int32, (2 * own, STRIP), 1), own)
                weights = jnp.where(query >= lax.broadcasted_iota(jnp.int32, (2 * own, STRIP), 0), weights, HIDDEN)
                top = weights.max(axis=0, keepdims=True)
            else:
                old = top_s[:, here]
                top = jnp.maximum(old, jnp.maximum(most[:1, here], most[1:2, here]))
                keep = jnp.exp2(old - top)
            top_s[:, here] = top
            got = _dot(values, jnp.exp2(weights - top).astype(jnp.bfloat16))
            total = got if first_step else acc[:, here] * keep + got
            if k == last if isinstance(k, int) else False:
                finish(total, c)
            else:
                acc[:, here] = total

    def finish(total, c):
        for h in range(STRIP // own):
            of = slice(h * own, (h + 1) * own)
            out = total[:HEAD, of] * (1 / total[HEAD : HEAD + 1, of])
            at_head = (c // own + h) * HEAD
            out_ref[:, at_head : at_head + HEAD] = out.T.astype(jnp.bfloat16)


    def other_block(k):
        return 2 * chip_of(k) + 1 - core

    arrived(partner, 20)
    scores(0, s_a, m_a)
    exchange(1)
    exchange(2)
    attend(0, s_a, m_a)
    exchange(3)
    exchange(4)
    pl.when(chip_of(1) < chip)(lambda: arrived(other_block(1), 21))
    scores(1, s_b, m_b)

    def pass_on(k, steps):
        for table, work in ((TAKEN, exchange), (SENT, sent)):
            for n, which in table.items():
                if n in steps:
                    @pl.when(k == n)
                    def _():
                        for r in which:
                            work(r)

    def wait_for(k):
        pl.when(chip_of(k) < chip)(lambda: arrived(other_block(k), 20 + k))

    def step(k, now, later):
        seen, ahead = chip_of(k) < chip, chip_of(k + 1) < chip

        @pl.when(seen)
        def _():
            scores(k + 1, *later)
            attend(k, *now)

        @pl.when(ahead & ~seen)
        def _():
            scores(k + 1, *later)

    even, uneven = (s_a, m_a), (s_b, m_b)

    def pair(t, _):
        for odd in (0, 1):
            k = 1 + odd + 2 * t
            pass_on(k, range(1 + odd, SINGLE + 1, 2))
            wait_for(k + 1)
            step(k, *((even, uneven) if odd else (uneven, even)))
        return _

    def double(t, _):
        k = SINGLE + 1 + 2 * t
        pass_on(k, range(SINGLE + 1, last, 2))
        wait_for(k + 1)
        wait_for(k + 2)
        whole = (chip_of(k) < chip) & (chip_of(k + 1) < chip)

        @pl.when(whole)
        def _():
            scores(k + 1, *even)
            attend(k, *uneven)
            scores(k + 2, *uneven)
            attend(k + 1, *even)

        @pl.when(~whole)
        def _():
            step(k, uneven, even)
            step(k + 1, even, uneven)

        return _

    lax.fori_loop(0, SINGLE // 2, pair, None)
    lax.fori_loop(0, (last - 1 - SINGLE) // 2, double, None)
    pl.when(chip_of(last) < chip)(functools.partial(attend, last, s_b, m_b))

    @pl.when(chip_of(last) >= chip)
    def _():
        for c in strips:
            finish(acc[:, c : c + STRIP], c)

    load_o.wait()
    for k in range(len(ORDER)):
        if all(k not in done for done in SENT.values()):
            sent(k)


def _finish(a_ref, x_ref, wo_ref, y_hbm, y_v, out_sem):
    def result(n):
        here = pl.ds(n * WIDE, WIDE)
        return pltpu.make_async_copy(y_v.at[:, here], y_hbm.at[:, here], out_sem.at[n])

    chunks = range(x_ref.shape[1] // WIDE)
    for n in chunks:
        here = slice(n * WIDE, (n + 1) * WIDE)
        y_v[:, here] = (x_ref[:, here].astype(jnp.float32) + _dot(a_ref[...], wo_ref[:, here])).astype(jnp.bfloat16)
        result(n).start()
    for n in chunks:
        result(n).wait()


def solution(mesh):
    side = math.isqrt(mesh.shape["sp"] // 2)
    assert 2 * side * side == mesh.shape["sp"] and side == 4

    def step(x, gain, wq, wk, wv, wo):
        own, d = x.shape
        heads = wq.shape[1] // HEAD
        cols = heads * own
        n = mesh.shape["sp"]
        hbm, vmem = pl.BlockSpec(memory_space=pltpu.HBM), pl.BlockSpec(memory_space=pltpu.VMEM)
        bf16, f32 = jnp.bfloat16, jnp.float32
        x_h, wq_h, wk_h, wv_h, wo_h = (pltpu.with_memory_space_constraint(t, pltpu.HBM) for t in (x, wq, wk, wv, wo))
        gain_h = pltpu.with_memory_space_constraint(gain, pltpu.HBM)
        attended, x_in, wo_in = pl.pallas_call(
            functools.partial(_kernel, side, heads),
            in_specs=[hbm] * 6,
            out_specs=[vmem, vmem, vmem],
            out_shape=[jax.ShapeDtypeStruct((own, cols), bf16), jax.ShapeDtypeStruct((own, d), bf16), jax.ShapeDtypeStruct(wo.shape, bf16)],
            scratch_shapes=[
                pltpu.VMEM((own, d), bf16),
                pltpu.VMEM(wq.shape, bf16),
                pltpu.VMEM((d, 2 * HEAD), bf16),
                pltpu.VMEM((HEAD, cols), bf16),
                pltpu.VMEM((n, 2, own, HEAD), bf16),
                pltpu.VMEM((HEAD + 8, cols), f32),
                pltpu.VMEM((1, cols), f32),
                pltpu.VMEM((2 * own, cols), f32),
                pltpu.VMEM((2 * own, cols), f32),
                pltpu.VMEM((2, cols), f32),
                pltpu.VMEM((2, cols), f32),
                pltpu.VMEM((own, HEAD // 2), f32),
                pltpu.VMEM((own, HEAD // 2), f32),
                pltpu.VMEM((d,), bf16),
                pltpu.SemaphoreType.DMA((9,)),
                pltpu.SemaphoreType.DMA((28,)),
                pltpu.SemaphoreType.DMA((20 + len(CHIPS),)),
            ],
            cost_estimate=pl.CostEstimate(flops=4 * cols * n * own * HEAD, bytes_accessed=2 * wq.size, transcendentals=0),
            compiler_params=pltpu.CompilerParams(collective_id=0, has_side_effects=True, vmem_limit_bytes=VMEM),
        )(x_h, gain_h, wq_h, wk_h, wv_h, wo_h)
        return pl.pallas_call(
            _finish,
            in_specs=[vmem, vmem, vmem],
            out_specs=hbm,
            out_shape=jax.ShapeDtypeStruct((own, d), bf16),
            scratch_shapes=[pltpu.VMEM((own, d), bf16), pltpu.SemaphoreType.DMA((d // WIDE,))],
            compiler_params=pltpu.CompilerParams(vmem_limit_bytes=16 * 2**20),
            cost_estimate=pl.CostEstimate(flops=2 * own * d * cols, bytes_accessed=2 * own * d, transcendentals=0),
        )(attended, x_in, wo_in)

    tokens, whole = P(("dp", "sp"), None), P(None, None)
    return jax.shard_map(step, mesh=mesh, in_specs=(tokens, P(None), whole, whole, whole, whole), out_specs=tokens, check_vma=False)
```

```python
import functools
import math

import jax
import jax.numpy as jnp
import numpy as np
from jax import lax
from jax.experimental import pallas as pl
from jax.experimental.pallas import tpu as pltpu
from jax.sharding import PartitionSpec as P

HEAD = 256
THETA = 10000
NEG = -1e30
HIDDEN = 2 * NEG
LOG2E = 1.4426950408889634
MESH = pl.DeviceIdType.MESH
VMEM = 38 * 2**20
STRIP = 512
WIDE = 512

ORDER = ((0, 0), (-1, 0), (1, 0), (0, -1), (0, 1), (2, 0), (-1, -1), (-1, 1), (1, -1), (1, 1), (0, 2), (2, -1), (2, 1), (-1, 2), (1, 2), (2, 2))
CHIPS = ((0, 0), (-1, 0), (0, -1), (1, 0), (0, 1), (-1, -1), (-1, 1), (1, -1), (1, 1), (2, 0), (0, 2), (2, -1), (-1, 2), (2, 1), (1, 2), (2, 2))
TAKEN = {2: (6,), 3: (7, 5), 4: (8,), 5: (9,), 6: (10,), 8: (11,), 9: (12, 13), 10: (14,), 12: (15,)}
SENT = {5: (0,), 7: (1, 2, 3, 4), 10: (5, 6, 7), 12: (8, 9, 10), 13: (11, 12, 13, 14)}
SINGLE = 12


RANK = {(a % 4, b % 4): k for k, (a, b) in enumerate(ORDER)}
STEP = {(x % 4, y % 4): k for k, (x, y) in enumerate(CHIPS)}
HALVED = (5, 10, 13, 14, 15)
BASE = (0, 5, 9, 13, 15, 17, 20, 22, 24, 26, 0, 5, 9, 13, 15, 17)


def _landing(k, half):
    return k - 1 if half != 1 else len(ORDER) - 1 + HALVED.index(k)


def _dot(a, b, ca=1, cb=0):
    return lax.dot_general(a, b, (((ca,), (cb,)), ((), ())), preferred_element_type=jnp.float32)


def _rope(t, cos, sin):
    half = t.shape[-1] // 2
    t = t.astype(jnp.bfloat16).astype(jnp.float32)
    a, b = t[:, :half], t[:, half:]
    return jnp.concatenate([a * cos - b * sin, b * cos + a * sin], -1)


def _kernel(side, heads, x_hbm, gain_hbm, wq_hbm, wk_hbm, wv_hbm, wo_hbm, out_ref, x_v, wo_v,
            a_v, wq_v, wkv_v, q_v, blk, acc, top_s, s_a, s_b, m_a, m_b, cos_v, sin_v, gain_v,
            in_sem, ssem, rsem):
    own, d = x_v.shape
    cols = heads * own
    e = HEAD**-0.5 * LOG2E
    me = lax.axis_index("sp")
    around = side - 1
    bits = around.bit_length()
    core = me & 1
    chip = me >> 1
    cx, cy = chip >> bits, chip & around
    p = cx + (cy - cx) * core
    s = cy + (cx - cy) * core
    wide = 2 * side
    wp, ws = wide - (wide - 2) * core, 2 + (wide - 2) * core
    partner = me + 1 - 2 * core

    def at(a, b):
        return ((p + a) & around) * wp + ((s + b) & around) * ws + core

    def chip_at(x, y):
        return (((cx + x) & around) << bits) + ((cy + y) & around)

    def chip_of(k):
        if isinstance(k, int):
            return chip_at(*CHIPS[k])
        x, y = (np.array([sum((c[n] % side) << bits * i for i, c in enumerate(CHIPS))]).astype(np.uint32).view(np.int32)[0].item() for n in (0, 1))
        digit = lambda packed: lax.shift_right_logical(jnp.int32(packed), jnp.int32(bits) * k) & around
        return chip_at(digit(x), digit(y))

    right_p, left_p, right_s, left_s = at(1, 0), at(-1, 0), at(0, 1), at(0, -1)

    load_x = pltpu.make_async_copy(x_hbm, x_v, in_sem.at[0])
    load_k = pltpu.make_async_copy(wk_hbm, wkv_v.at[:, pl.ds(0, HEAD)], in_sem.at[1])
    load_v = pltpu.make_async_copy(wv_hbm, wkv_v.at[:, pl.ds(HEAD, HEAD)], in_sem.at[2])

    load_o = pltpu.make_async_copy(wo_hbm, wo_v, in_sem.at[3])

    def load_q(n):
        here = pl.ds(n * WIDE if isinstance(n, int) else pl.multiple_of(n * WIDE, WIDE), WIDE)
        return pltpu.make_async_copy(wq_hbm.at[:, here], wq_v.at[:, here], in_sem.at[4 + n])

    load_g = pltpu.make_async_copy(gain_hbm, gain_v, in_sem.at[8])
    load_x.start()
    load_g.start()
    load_k.start()
    load_v.start()
    barrier = pltpu.get_barrier_semaphore()
    for other in (right_p, left_p, right_s, left_s, partner):
        pl.semaphore_signal(barrier, inc=1, device_id={"sp": other}, device_id_type=MESH)

    place = (me * own + lax.broadcasted_iota(jnp.int32, (own, HEAD // 2), 0)).astype(jnp.float32)
    half = HEAD // 2
    angle = place * jnp.exp2(lax.broadcasted_iota(jnp.int32, (1, half), 1).astype(jnp.float32) * (-math.log2(THETA) / half))
    cos_v[...] = jnp.cos(angle)
    sin_v[...] = jnp.sin(angle)

    load_x.wait()
    load_g.wait()
    for n in range(cols // WIDE):
        load_q(n).start()
    x = x_v[...].astype(jnp.float32)
    scale = lax.rsqrt(jnp.mean(x * x, -1, keepdims=True) + 1e-6)
    a_v[...] = (x * scale * gain_v[...].astype(jnp.float32)[None]).astype(jnp.bfloat16)
    load_k.wait()
    load_v.wait()
    kv = _dot(a_v[...], wkv_v[...])
    blk[me, 0] = _rope(kv[:, :HEAD], cos_v[...], sin_v[...]).astype(jnp.bfloat16)
    blk[me, 1] = kv[:, HEAD:].T.astype(jnp.bfloat16)

    def line_end(n):
        return ((p + n) & around) * (side - around * core) + around * (1 + around * core)

    def along(n):
        return at(0, n) >> 1

    def arrives(k):
        (a, b), of = ORDER[k], at(*ORDER[k]) >> 1
        if b == 0:
            return line_end(0) > of if a == 2 else (line_end(0) > of) | (line_end(-a) > of)
        return along(0) > of if b == 2 else (along(0) > of) | (along(-b) > of)

    def sends_of(k):
        (a, b), of = ORDER[k], at(*ORDER[k]) >> 1
        x, y = STEP[a % 4, b % 4], STEP[b % 4, a % 4]
        out = [(along(0) > of if k else None, None, partner, 20 + x + (y - x) * core)]
        if b == 0:
            out += [((along(n) > of) | (along(2) > of), None, at(0, n), _landing(RANK[a % 4, (b - n) % 4], None)) for n in (1, -1)]
        elif b != 2:
            half = 0 if b < 0 else 1
            out += [(along(-b) > of, half, at(0, -b), _landing(RANK[a % 4, 2], half))]
        if k == 0:
            out += [((line_end(n) > of) | (line_end(2) > of), None, at(n, 0), _landing(RANK[-n % 4, 0], None)) for n in (1, -1)]
        elif b == 0 and a != 2:
            half = 0 if a < 0 else 1
            out += [(line_end(-a) > of, half, at(-a, 0), _landing(RANK[2, 0], half))]
        return out

    def copy_of(block, part, other, send, landing):
        ref = blk.at[block] if part is None else blk.at[block, part]
        return pltpu.make_async_remote_copy(src_ref=ref, dst_ref=ref, send_sem=ssem.at[send], recv_sem=rsem.at[landing],
                                            device_id={"sp": other}, device_id_type=MESH)

    def send(k, which):
        block, todo = at(*ORDER[k]), sends_of(k)
        for n in which if which else range(len(todo)):
            whether, part, other, landing = todo[n]
            copy = copy_of(block, part, other, BASE[k] + n, landing)
            copy.start() if whether is None else pl.when(whether)(copy.start)

    def sent(k):
        for n, (whether, part, other, landing) in enumerate(sends_of(k)):
            copy = copy_of(me, part, other, BASE[k] + n, landing)
            copy.wait_send() if whether is None else pl.when(whether)(copy.wait_send)

    def arrived(block, landing, part=None):
        copy_of(block, part, partner, 0, landing).wait_recv()

    pl.semaphore_wait(barrier, 5)
    send(0, (3, 4))

    def project(n, _):
        load_q(n).wait()
        here = pl.ds(pl.multiple_of(n * WIDE, WIDE), WIDE)
        q = _dot(a_v[...], wq_v[:, here])
        for h in range(WIDE // HEAD):
            turned = _rope(q[:, h * HEAD : (h + 1) * HEAD], cos_v[...], sin_v[...])
            q_v[:, pl.ds(pl.multiple_of(n * WIDE + h * HEAD, HEAD), HEAD)] = turned.T.astype(jnp.bfloat16)
        return _

    lax.fori_loop(0, 1, project, None)
    send(0, (0,))
    lax.fori_loop(1, cols // WIDE - 1, project, None)
    load_o.start()
    send(0, (1, 2))
    lax.fori_loop(cols // WIDE - 1, cols // WIDE, project, None)

    def exchange(k):
        a, b = ORDER[k]
        block = at(a, b)

        @pl.when(arrives(k))
        def _():
            for half in (0, 1) if k in HALVED else (None,):
                arrived(block, _landing(k, half), half)

        if k in (1, 2):
            send(k, (1, 2, 0))
        else:
            send(k, None)
        if k == 4:
            send(1, (3,))
            send(2, (3,))

    strips = range(0, cols, STRIP)
    last = len(CHIPS) - 1

    def scores(k, out, most):
        chip = chip_of(k)
        for n in (0, 1):
            for c in strips:
                sc = _dot(blk[2 * chip + n, 0], q_v[:, c : c + STRIP]) * e
                out[n * own : (n + 1) * own, c : c + STRIP] = sc
                most[n : n + 1, c : c + STRIP] = sc.max(axis=0, keepdims=True)

    def attend(k, sc, most):
        chip = chip_of(k)
        values = jnp.concatenate([blk[2 * chip, 1], blk[2 * chip + 1, 1]], axis=1)
        values = jnp.concatenate([values, jnp.ones((8, 2 * own), jnp.bfloat16)], axis=0)
        first_step = isinstance(k, int) and k == 0
        for c in strips:
            here = slice(c, c + STRIP)
            weights = sc[:, here]
            if first_step:
                query = core * own + lax.rem(lax.broadcasted_iota(jnp.int32, (2 * own, STRIP), 1), own)
                weights = jnp.where(query >= lax.broadcasted_iota(jnp.int32, (2 * own, STRIP), 0), weights, HIDDEN)
                top = weights.max(axis=0, keepdims=True)
            else:
                old = top_s[:, here]
                top = jnp.maximum(old, jnp.maximum(most[:1, here], most[1:2, here]))
                keep = jnp.exp2(old - top)
            top_s[:, here] = top
            got = _dot(values, jnp.exp2(weights - top).astype(jnp.bfloat16))
            total = got if first_step else acc[:, here] * keep + got
            if k == last if isinstance(k, int) else False:
                finish(total, c)
            else:
                acc[:, here] = total

    def finish(total, c):
        for h in range(STRIP // own):
            of = slice(h * own, (h + 1) * own)
            out = total[:HEAD, of] * (1 / total[HEAD : HEAD + 1, of])
            at_head = (c // own + h) * HEAD
            out_ref[:, at_head : at_head + HEAD] = out.T.astype(jnp.bfloat16)


    def other_block(k):
        return 2 * chip_of(k) + 1 - core

    arrived(partner, 20)
    scores(0, s_a, m_a)
    exchange(1)
    exchange(2)
    attend(0, s_a, m_a)
    exchange(3)
    exchange(4)
    pl.when(chip_of(1) < chip)(lambda: arrived(other_block(1), 21))
    scores(1, s_b, m_b)

    def pass_on(k, steps):
        for table, work in ((TAKEN, exchange), (SENT, sent)):
            for n, which in table.items():
                if n in steps:
                    @pl.when(k == n)
                    def _():
                        for r in which:
                            work(r)

    def wait_for(k):
        pl.when(chip_of(k) < chip)(lambda: arrived(other_block(k), 20 + k))

    def step(k, now, later):
        seen, ahead = chip_of(k) < chip, chip_of(k + 1) < chip

        @pl.when(seen)
        def _():
            scores(k + 1, *later)
            attend(k, *now)

        @pl.when(ahead & ~seen)
        def _():
            scores(k + 1, *later)

    even, uneven = (s_a, m_a), (s_b, m_b)

    def pair(t, _):
        for odd in (0, 1):
            k = 1 + odd + 2 * t
            pass_on(k, range(1 + odd, SINGLE + 1, 2))
            wait_for(k + 1)
            step(k, *((even, uneven) if odd else (uneven, even)))
        return _

    def double(t, _):
        k = SINGLE + 1 + 2 * t
        pass_on(k, range(SINGLE + 1, last, 2))
        wait_for(k + 1)
        wait_for(k + 2)
        whole = (chip_of(k) < chip) & (chip_of(k + 1) < chip)

        @pl.when(whole)
        def _():
            scores(k + 1, *even)
            attend(k, *uneven)
            scores(k + 2, *uneven)
            attend(k + 1, *even)

        @pl.when(~whole)
        def _():
            step(k, uneven, even)
            step(k + 1, even, uneven)

        return _

    lax.fori_loop(0, SINGLE // 2, pair, None)
    lax.fori_loop(0, (last - 1 - SINGLE) // 2, double, None)
    pl.when(chip_of(last) < chip)(functools.partial(attend, last, s_b, m_b))

    @pl.when(chip_of(last) >= chip)
    def _():
        for c in strips:
            finish(acc[:, c : c + STRIP], c)

    load_o.wait()
    for k in range(len(ORDER)):
        if all(k not in done for done in SENT.values()):
            sent(k)


def _finish(a_ref, x_ref, wo_ref, y_hbm, y_v, out_sem):
    d = x_ref.shape[1]
    edges = [*range(0, d, WIDE), d - WIDE // 2, d]

    def result(n):
        here = pl.ds(edges[n], edges[n + 1] - edges[n])
        return pltpu.make_async_copy(y_v.at[:, here], y_hbm.at[:, here], out_sem.at[n])

    chunks = range(len(edges) - 1)
    for n in chunks:
        here = slice(edges[n], edges[n + 1])
        y_v[:, here] = (x_ref[:, here].astype(jnp.float32) + _dot(a_ref[...], wo_ref[:, here])).astype(jnp.bfloat16)
        result(n).start()
    for n in chunks:
        result(n).wait()


def solution(mesh):
    side = math.isqrt(mesh.shape["sp"] // 2)
    assert 2 * side * side == mesh.shape["sp"] and side == 4

    def step(x, gain, wq, wk, wv, wo):
        own, d = x.shape
        heads = wq.shape[1] // HEAD
        cols = heads * own
        n = mesh.shape["sp"]
        hbm, vmem = pl.BlockSpec(memory_space=pltpu.HBM), pl.BlockSpec(memory_space=pltpu.VMEM)
        bf16, f32 = jnp.bfloat16, jnp.float32
        x_h, wq_h, wk_h, wv_h, wo_h = (pltpu.with_memory_space_constraint(t, pltpu.HBM) for t in (x, wq, wk, wv, wo))
        gain_h = pltpu.with_memory_space_constraint(gain, pltpu.HBM)
        attended, x_in, wo_in = pl.pallas_call(
            functools.partial(_kernel, side, heads),
            in_specs=[hbm] * 6,
            out_specs=[vmem, vmem, vmem],
            out_shape=[jax.ShapeDtypeStruct((own, cols), bf16), jax.ShapeDtypeStruct((own, d), bf16), jax.ShapeDtypeStruct(wo.shape, bf16)],
            scratch_shapes=[
                pltpu.VMEM((own, d), bf16),
                pltpu.VMEM(wq.shape, bf16),
                pltpu.VMEM((d, 2 * HEAD), bf16),
                pltpu.VMEM((HEAD, cols), bf16),
                pltpu.VMEM((n, 2, own, HEAD), bf16),
                pltpu.VMEM((HEAD + 8, cols), f32),
                pltpu.VMEM((1, cols), f32),
                pltpu.VMEM((2 * own, cols), f32),
                pltpu.VMEM((2 * own, cols), f32),
                pltpu.VMEM((2, cols), f32),
                pltpu.VMEM((2, cols), f32),
                pltpu.VMEM((own, HEAD // 2), f32),
                pltpu.VMEM((own, HEAD // 2), f32),
                pltpu.VMEM((d,), bf16),
                pltpu.SemaphoreType.DMA((9,)),
                pltpu.SemaphoreType.DMA((28,)),
                pltpu.SemaphoreType.DMA((20 + len(CHIPS),)),
            ],
            cost_estimate=pl.CostEstimate(flops=4 * cols * n * own * HEAD, bytes_accessed=2 * wq.size, transcendentals=0),
            compiler_params=pltpu.CompilerParams(collective_id=0, has_side_effects=True, vmem_limit_bytes=VMEM),
        )(x_h, gain_h, wq_h, wk_h, wv_h, wo_h)
        return pl.pallas_call(
            _finish,
            in_specs=[vmem, vmem, vmem],
            out_specs=hbm,
            out_shape=jax.ShapeDtypeStruct((own, d), bf16),
            scratch_shapes=[pltpu.VMEM((own, d), bf16), pltpu.SemaphoreType.DMA((d // WIDE + 1,))],
            compiler_params=pltpu.CompilerParams(vmem_limit_bytes=16 * 2**20),
            cost_estimate=pl.CostEstimate(flops=2 * own * d * cols, bytes_accessed=2 * own * d, transcendentals=0),
        )(attended, x_in, wo_in)

    tokens, whole = P(("dp", "sp"), None), P(None, None)
    return jax.shard_map(step, mesh=mesh, in_specs=(tokens, P(None), whole, whole, whole, whole), out_specs=tokens, check_vma=False)
```
